128 devices in a mesh: tile: 64 (over x, z, y), lev: 2 (over core).
Axes of the slice: x: 4, y: 4, z: 4, core: 2. Of those that a mesh axis runs over, the one named last changes fastest.
Arguments:
- increments: bfloat16 [136, 1024, 1024], P('lev', 'tile'), may hold values from -30 to 30
- projection: bfloat16 [80, 136], replicated, may hold values from -0.5 to 0.5
- helmholtz: float32 [80], P('lev'), may hold values from 0.05 to 4
Outputs:
- solution: float32 [80, 1024, 1024], P('lev', 'tile')
- residual: float32 [80, 1024, 1024], P('lev', 'tile')
The draws below stay inside these ranges and needn't reach their ends.
All inputs are finite; a program needn't handle non-finite values.
Results may differ from the reference program's by a relative error of at most 0.00075.
Values may be sent and summed in bfloat16 or wider, within the bound.
No kernel may reach another device: no remote copies, remote signals or barrier semaphores. Data moves between devices by JAX's collectives and lax.ppermute only.
A program may use at most 192 MiB of HBM per device.

```python
import math
import jax
import jax.numpy as jnp
import numpy as np
from jax import lax

LEVELS = 136
MODES = 80
S = 4
BLOCKS = 2
NY = 1024
NX = 1024


def lowpass(field):
    for repeat in range(2):
        field = 0.25 * (jnp.roll(field, 1, 1) + 2.0 * field + jnp.roll(field, -1, 1))
        field = 0.25 * (jnp.roll(field, 1, 2) + 2.0 * field + jnp.roll(field, -1, 2))
    return field


def draw_increments(key, part):
    key_base = jax.random.fold_in(key, 11)
    key_one, key_two = jax.random.split(key_base, 2)
    row_frac = (jnp.arange(NX, dtype=jnp.float32) / NX)[None, :, None]
    base = jnp.clip(jax.random.normal(key_one, (LEVELS, NX, NY), jnp.float32), -6.0, 6.0)
    smooth = lowpass(jnp.clip(jax.random.normal(key_two, (LEVELS, NX, NY), jnp.float32), -6.0, 6.0))
    values = base + 10.0 * row_frac * smooth
    return jnp.clip(values, -30.0, 30.0).astype(jnp.bfloat16)


def levels(stream_key, dims, cuts, least, high):
    loudness, own = 1.0, jax.random.fold_in(stream_key, 6)
    for axis_at, blocks in cuts:
        steps = jnp.exp(jax.random.uniform(jax.random.fold_in(own, axis_at), (blocks,), jnp.float32, least / len(cuts), high / len(cuts)))
        loudness = loudness * jnp.repeat(steps, dims[axis_at] // blocks).reshape([-1 if axis == axis_at else 1 for axis in range(len(dims))])
    return loudness


def normal_values(key, extent, deviation, bound, held_as=jnp.bfloat16):
    entries = deviation * jax.random.normal(key, extent, jnp.float32)
    return jnp.clip(entries, min=-bound, max=bound).astype(held_as)


def setup_inputs(seed: int = 0) -> dict:
    streams_of = jax.random.split(jax.random.key(seed), 4)
    increments = draw_increments(jax.random.fold_in(streams_of[3], 71), 0)
    projection = normal_values(streams_of[1], (MODES, LEVELS), LEVELS ** -0.5, 0.5)
    helmholtz = jnp.clip(jnp.exp(math.log(4.0) - 4.3820266 * jax.random.uniform(streams_of[2], (MODES,), jnp.float32) ** levels(streams_of[2], (MODES,), ((0, 2),), -0.2, 0.2)), 0.05, 4.0)
    return dict(increments=increments, projection=projection, helmholtz=helmholtz)


highest = lax.Precision.HIGHEST


def stencil(field, weight):
    padded = jnp.pad(field, 1)
    beside_all = padded[2:, 1:-1] + padded[:-2, 1:-1] + padded[1:-1, 2:] + padded[1:-1, :-2]
    return weight * beside_all


def shift_matrix():
    width = 2 * S + 1
    table = np.zeros((width, width), np.float32)
    for index in range(S):
        table[index + 1, index] = 1.0
    for index in range(S - 1):
        table[S + 2 + index, S + 1 + index] = 1.0
    return jnp.asarray(table, jnp.float32)


def quadratic(gram, left, right):
    return jnp.dot(left, jnp.dot(gram, right, precision=highest), precision=highest)


def solve_mode(inputs):
    rhs, weight = inputs
    width = 2 * S + 1
    shifter = shift_matrix()
    solution = jnp.zeros_like(rhs)
    resid = rhs
    direction = rhs
    for block_index in range(BLOCKS):
        vectors = [direction]
        current = direction
        for power_index in range(S):
            current = stencil(current, weight)
            vectors.append(current)
        vectors.append(resid)
        current = resid
        for power_index in range(S - 1):
            current = stencil(current, weight)
            vectors.append(current)
        basis = jnp.stack(vectors).reshape(width, -1)
        gram = jnp.dot(basis, basis.T, precision=highest)
        p_coef = jnp.zeros((width,), jnp.float32).at[0].set(1.0)
        r_coef = jnp.zeros((width,), jnp.float32).at[S + 1].set(1.0)
        x_coef = jnp.zeros((width,), jnp.float32)
        squares = quadratic(gram, r_coef, r_coef)
        for step_index in range(S):
            moved = p_coef - jnp.dot(shifter, p_coef, precision=highest)
            alpha = squares / quadratic(gram, p_coef, moved)
            x_coef = x_coef + alpha * p_coef
            r_coef = r_coef - alpha * moved
            fresh = quadratic(gram, r_coef, r_coef)
            p_coef = r_coef + (fresh / squares) * p_coef
            squares = fresh
        solution = solution + jnp.dot(x_coef, basis, precision=highest).reshape(rhs.shape)
        resid = jnp.dot(r_coef, basis, precision=highest).reshape(rhs.shape)
        direction = jnp.dot(p_coef, basis, precision=highest).reshape(rhs.shape)
    return solution, resid


def reference(increments, projection, helmholtz):
    flat = increments.reshape(LEVELS, NX * NY)
    modal = jnp.dot(projection, flat, preferred_element_type=jnp.float32).reshape(MODES, NX, NY)
    weights = 1.0 / (4.0 + helmholtz)
    solution, resid = lax.map(solve_mode, (modal, weights))
    return solution, resid
```

```python
import functools

import jax
import jax.numpy as jnp
from jax import lax
from jax.experimental import pallas as pl
from jax.experimental.pallas import tpu as pltpu
from jax.sharding import PartitionSpec as P

STEPS = 8
MOMENTS = 2 * STEPS + 1
ROWS = 16
HALO = 8
MODES = 40
GROUPS = 5
LANES = 128
COLS = 1024
BLOCKS = COLS // LANES
TILES = 64
CODE_BITS = 31
CODE = 2.0 ** CODE_BITS

f32 = jnp.float32
bf16 = jnp.bfloat16


def limits(mib):
    return pltpu.CompilerParams(vmem_limit_bytes=mib * 2**20)


def build_left(proj_ref, left_ref, level0):
    lev = lax.axis_index("lev")
    depth = left_ref.shape[1]
    pick = (
        lax.broadcasted_iota(jnp.int32, (MODES, 2 * MODES), 1)
        == lax.broadcasted_iota(jnp.int32, (MODES, 2 * MODES), 0) + lev * MODES
    ).astype(bf16)
    own = jnp.dot(pick, proj_ref[...], preferred_element_type=f32).astype(bf16)
    levels = proj_ref.shape[1]
    spread = (
        lax.broadcasted_iota(jnp.int32, (levels, depth), 0)
        == (lax.broadcasted_iota(jnp.int32, (levels, depth), 1) >> 4) + level0
    ).astype(bf16)
    wide = jnp.dot(own, spread, preferred_element_type=f32)
    row_of = lax.broadcasted_iota(jnp.int32, (8, depth), 1) & (ROWS - 1)
    for group in range(GROUPS):
        part = wide[group * 8:(group + 1) * 8]
        for row in range(0, ROWS, 2):
            two = jnp.concatenate(
                [jnp.where(row_of == row, part, 0.0), jnp.where(row_of == row + 1, part, 0.0)],
                axis=0,
            )
            at = group * 8 * ROWS + row * 8
            left_ref[at:at + 16, :] = two.astype(bf16)


def own_levels_kernel(proj_ref, inc_ref, acc_ref, other_left_ref, left_ref):
    lev = lax.axis_index("lev")
    count = proj_ref.shape[1] // 2

    @pl.when(pl.program_id(0) == 0)
    def _():
        build_left(proj_ref, left_ref, lev * count)
        build_left(proj_ref, other_left_ref, (1 - lev) * count)

    acc_ref[...] = jnp.dot(left_ref[...], inc_ref[...], preferred_element_type=f32)


def other_levels_kernel(left_ref, inc_ref, acc_ref, modal_ref, a_ref, b_ref):
    even = (lax.axis_index("tile") & 1) == 0
    modal_ref[...] = acc_ref[...] + jnp.dot(
        left_ref[...], inc_ref[...], preferred_element_type=f32
    )
    half = 8 * HALO
    for group in range(GROUPS):
        at = group * 2 * half
        low = modal_ref[at:at + half, :]
        high = modal_ref[at + half:at + 2 * half, :]
        for ref, value in (
            (a_ref, jnp.where(even, high, low)),
            (b_ref, jnp.where(even, low, high)),
        ):
            scaled = value * CODE
            ref[group * half:(group + 1) * half, :] = (scaled * scaled * scaled).astype(bf16)


def modal_product(increments, projection):
    levels = increments.shape[0]
    depth = levels * ROWS
    flat = increments.reshape(depth, COLS)
    arrived = lax.ppermute(flat, "lev", [(0, 1), (1, 0)])
    width = 256
    grid = (COLS // width,)
    total = MODES * ROWS
    acc, other_left = pl.pallas_call(
        own_levels_kernel,
        grid=grid,
        in_specs=[
            pl.BlockSpec(projection.shape, lambda c: (0, 0)),
            pl.BlockSpec((depth, width), lambda c: (0, c)),
        ],
        out_specs=[
            pl.BlockSpec((total, width), lambda c: (0, c)),
            pl.BlockSpec((total, depth), lambda c: (0, 0)),
        ],
        out_shape=[
            jax.ShapeDtypeStruct((total, COLS), f32),
            jax.ShapeDtypeStruct((total, depth), bf16),
        ],
        scratch_shapes=[pltpu.VMEM((total, depth), bf16)],
        compiler_params=limits(20),
        name="own_levels",
    )(projection, flat)
    half = total // 2
    return pl.pallas_call(
        other_levels_kernel,
        grid=grid,
        in_specs=[
            pl.BlockSpec((total, depth), lambda c: (0, 0)),
            pl.BlockSpec((depth, width), lambda c: (0, c)),
            pl.BlockSpec((total, width), lambda c: (0, c)),
        ],
        out_specs=[
            pl.BlockSpec((total, width), lambda c: (0, c)),
            pl.BlockSpec((half, width), lambda c: (0, c)),
            pl.BlockSpec((half, width), lambda c: (0, c)),
        ],
        out_shape=[
            jax.ShapeDtypeStruct((total, COLS), f32),
            jax.ShapeDtypeStruct((half, COLS), bf16),
            jax.ShapeDtypeStruct((half, COLS), bf16),
        ],
        compiler_params=limits(20),
        name="other_levels",
    )(other_left, arrived, acc)


def decoded(value):
    value = value.astype(f32)
    root = jnp.exp2(jnp.log2(jnp.abs(value)) * (1.0 / 3.0) - CODE_BITS)
    return jnp.where(value < 0.0, -root, root)


def basis_kernel(modal_ref, a_ref, b_ref, basis_ref, moment_ref, low_ref, high_ref, sums_ref):
    tile = lax.axis_index("tile")
    even = (tile & 1) == 0
    group = pl.program_id(0)
    for row in range(0, HALO, 2):
        part = slice(row * 8, row * 8 + 16)
        a = decoded(a_ref[part, :])
        b = decoded(b_ref[part, :])
        low_ref[0, part, :] = jnp.where(even, b, a)
        high_ref[0, part, :] = jnp.where(even, a, b)
    lane = lax.broadcasted_iota(jnp.int32, (8, LANES), 1)
    first = lane == 0
    last = lane == LANES - 1
    half_low = jnp.where(tile == 0, 0.0, 0.5)
    half_high = jnp.where(tile == TILES - 1, 0.0, 0.5)

    def load(order, row):
        if row < 0:
            at = (row + HALO) * 8
            return [low_ref[order % 3, at:at + 8, b * LANES:(b + 1) * LANES] for b in range(BLOCKS)]
        if row >= ROWS:
            at = (row - ROWS) * 8
            return [high_ref[order % 3, at:at + 8, b * LANES:(b + 1) * LANES] for b in range(BLOCKS)]
        at = row * 8
        if order == 0:
            return [modal_ref[at:at + 8, b * LANES:(b + 1) * LANES] for b in range(BLOCKS)]
        return [basis_ref[order - 1, at:at + 8, b * LANES:(b + 1) * LANES] for b in range(BLOCKS)]

    def store(order, row, values):
        for b, value in enumerate(values):
            cols = slice(b * LANES, (b + 1) * LANES)
            if row < 0:
                at = (row + HALO) * 8
                low_ref[order % 3, at:at + 8, cols] = value
            elif row >= ROWS:
                at = (row - ROWS) * 8
                high_ref[order % 3, at:at + 8, cols] = value
            else:
                basis_ref[order - 1, row * 8:row * 8 + 8, cols] = value

    def diagonal(field, below):
        turned = [pltpu.roll(v, LANES - 1, 1) for v in below]
        out = []
        for b in range(BLOCKS):
            edge = turned[b + 1] if b + 1 < BLOCKS else 0.0
            out.append(field[b] + jnp.where(last, edge, turned[b]))
        return out

    def total(values):
        while len(values) > 1:
            values = [values[i] + values[i + 1] for i in range(0, len(values), 2)]
        return values[0]

    square0 = jnp.zeros((8, LANES), f32)
    for order in range(1, STEPS + 1):
        square = jnp.zeros((8, LANES), f32)
        cross = jnp.zeros((8, LANES), f32)
        begin, end = order - HALO, ROWS + HALO - order
        before = load(order - 1, begin - 1)
        here = load(order - 1, begin)
        upper = diagonal(before, here)
        for row in range(begin, end):
            below = load(order - 1, row + 1)
            lower = diagonal(here, below)
            turned = [pltpu.roll(v, 1, 1) for v in lower]
            new = []
            if order == 1:
                factor = 0.25 if 0 <= row < ROWS else (half_low if row < 0 else half_high) * 0.5
                older = None
            else:
                factor = 0.5 if 0 <= row < ROWS else (half_low if row < 0 else half_high)
                older = load(order - 2, row)
            for b in range(BLOCKS):
                edge = turned[b - 1] if b else below[0]
                value = (upper[b] + jnp.where(first, edge, turned[b])) * factor
                if older is not None:
                    value = value - older[b]
                new.append(value)
            store(order, row, new)
            if 0 <= row < ROWS:
                square = square + total([v * v for v in new])
                cross = cross + total([v * w for v, w in zip(new, here)])
                if order == 1:
                    square0 = square0 + total([v * v for v in here])
            upper, here = lower, below
        if order == 1:
            sums_ref[0] = square0
        sums_ref[2 * order - 1] = cross
        sums_ref[2 * order] = square

    @pl.when(group == 0)
    def _():
        moment_ref[...] = jnp.zeros_like(moment_ref)

    packed = moment_ref[...]
    for index in range(MOMENTS):
        value = jnp.sum(sums_ref[index], axis=1, keepdims=True)
        packed = jnp.where(lane == index * GROUPS + group, value, packed)
    moment_ref[...] = packed


def basis_and_moments(modal, a, b):
    rows = 8 * ROWS
    halo = 8 * HALO
    return pl.pallas_call(
        basis_kernel,
        grid=(GROUPS,),
        in_specs=[
            pl.BlockSpec((rows, COLS), lambda g: (g, 0)),
            pl.BlockSpec((halo, COLS), lambda g: (g, 0)),
            pl.BlockSpec((halo, COLS), lambda g: (g, 0)),
        ],
        out_specs=[
            pl.BlockSpec((STEPS, rows, COLS), lambda g: (0, g, 0)),
            pl.BlockSpec((8, LANES), lambda g: (0, 0)),
        ],
        out_shape=[
            jax.ShapeDtypeStruct((STEPS, MODES * ROWS, COLS), f32),
            jax.ShapeDtypeStruct((8, LANES), f32),
        ],
        scratch_shapes=[
            pltpu.VMEM((3, halo, COLS), f32),
            pltpu.VMEM((3, halo, COLS), f32),
            pltpu.VMEM((MOMENTS, 8, LANES), f32),
        ],
        compiler_params=limits(20),
        name="basis",
    )(modal, a, b)


def coefficients(nu, tau):
    half = 0.5 * tau
    rho = list(nu)
    pi = list(nu)
    one, zero = jnp.ones_like(tau), None
    r = [one]
    p = [one]
    x = [None] * STEPS
    rr = nu[0]

    def plus(a, b):
        if a is None:
            return b
        if b is None:
            return a
        return a + b

    def inner(c, v):
        terms = [ci * vi for ci, vi in zip(c, v)]
        while len(terms) > 1:
            terms = [sum(terms[i:i + 2]) for i in range(0, len(terms), 2)]
        return terms[0]

    for step in range(STEPS):
        top = MOMENTS - 1 - step
        image = []
        for l in range(top):
            near = pi[l + 1] + pi[abs(l - 1)]
            image.append(pi[l] - half * near)
        alpha = rr / inner(p, image)
        x = [plus(x[i], alpha * p[i]) if i < len(p) else x[i] for i in range(STEPS)]
        shifted = [None] * (len(p) + 1)
        for k, value in enumerate(p):
            if k == 0:
                shifted[1] = plus(shifted[1], tau * value)
            else:
                scaled = half * value
                shifted[k + 1] = plus(shifted[k + 1], scaled)
                shifted[k - 1] = plus(shifted[k - 1], scaled)
        moved = []
        for k in range(len(p) + 1):
            own = p[k] if k < len(p) else None
            if shifted[k] is None:
                moved.append(own)
            elif own is None:
                moved.append(-shifted[k])
            else:
                moved.append(own - shifted[k])
        r = [
            (r[k] - alpha * moved[k]) if k < len(r) else -(alpha * moved[k])
            for k in range(len(moved))
        ]
        if step == STEPS - 1:
            break
        rho = [rho[l] - alpha * image[l] for l in range(top)]
        fresh = inner(r, rho)
        beta = fresh / rr
        pi = [rho[l] + beta * pi[l] for l in range(top)]
        p = [plus(r[k], beta * p[k] if k < len(p) else None) for k in range(len(r))]
        rr = fresh
    return x, r


def solve_kernel(sums_ref, helm_ref, modal_ref, basis_ref, x_ref, r_ref, coef_ref):
    group = pl.program_id(0)

    @pl.when(group == 0)
    def _():
        parts = [sums_ref[i] for i in range(TILES)]
        while len(parts) > 1:
            parts = [parts[i] + parts[i + 1] for i in range(0, len(parts), 2)]
        moments = parts[0]
        raw = [moments if k == 0 else pltpu.roll(moments, LANES - GROUPS * k, 1) for k in range(MOMENTS)]
        nu = raw[:2]
        for k in range(2, MOMENTS):
            nu.append(2.0 * raw[k] - nu[k & 1])
        tau = 4.0 / (4.0 + helm_ref[...])
        x, r = coefficients(nu, tau)
        for g in range(GROUPS):
            for k, value in enumerate(x + r):
                coef_ref[g, k] = jnp.broadcast_to(value[:, g:g + 1], (8, LANES))

    for b in range(BLOCKS):
        cols = slice(b * LANES, (b + 1) * LANES)
        cx = [coef_ref[group, k] for k in range(STEPS)]
        cr = [coef_ref[group, STEPS + k] for k in range(STEPS + 1)]
        for top in range(0, ROWS, 8):
            xs, rs = [], []
            for row in range(top, top + 8):
                at = slice(row * 8, row * 8 + 8)
                field = modal_ref[at, cols]
                x = cx[0] * field
                r = cr[0] * field
                for k in range(1, STEPS + 1):
                    field = basis_ref[k - 1, at, cols]
                    if k < STEPS:
                        x = x + cx[k] * field
                    r = r + cr[k] * field
                xs.append(x)
                rs.append(r)
            x_ref[:, top:top + 8, cols] = jnp.swapaxes(jnp.stack(xs), 0, 1)
            r_ref[:, top:top + 8, cols] = jnp.swapaxes(jnp.stack(rs), 0, 1)


def solve(sums, helm, modal, basis):
    rows = 8 * ROWS
    out = jax.ShapeDtypeStruct((MODES, ROWS, COLS), f32)
    return pl.pallas_call(
        solve_kernel,
        grid=(GROUPS,),
        in_specs=[
            pl.BlockSpec((TILES, 8, LANES), lambda g: (0, 0, 0)),
            pl.BlockSpec((8, LANES), lambda g: (0, 0)),
            pl.BlockSpec((rows, COLS), lambda g: (g, 0)),
            pl.BlockSpec((STEPS, rows, COLS), lambda g: (0, g, 0)),
        ],
        out_specs=[
            pl.BlockSpec((8, ROWS, COLS), lambda g: (g, 0, 0)),
            pl.BlockSpec((8, ROWS, COLS), lambda g: (g, 0, 0)),
        ],
        out_shape=[out, out],
        scratch_shapes=[pltpu.VMEM((GROUPS, MOMENTS, 8, LANES), f32)],
        compiler_params=limits(20),
        name="solve",
    )(sums, helm, modal, basis)


def shards(increments, projection, helmholtz):
    modal, a, b = modal_product(increments, projection)
    swap_a = [(i, i ^ 1) for i in range(TILES)]
    swap_b = [(i, i + 1) for i in range(1, TILES - 1, 2)]
    swap_b += [(target, source) for source, target in swap_b]
    a = lax.ppermute(a, "tile", swap_a)
    b = lax.ppermute(b, "tile", swap_b)
    basis, moments = basis_and_moments(modal, a, b)
    spread = jnp.broadcast_to(moments[None], (TILES, 8, LANES))
    sums = lax.all_to_all(spread, "tile", 0, 0, tiled=True)
    helm = jnp.pad(helmholtz.reshape(GROUPS, 8).T, ((0, 0), (0, LANES - GROUPS)))
    return tuple(solve(sums, helm, modal, basis))


def solution(mesh):
    in_specs = (P("lev", "tile", None), P(), P("lev"))
    out_specs = (P("lev", "tile", None), P("lev", "tile", None))
    return jax.shard_map(shards, mesh=mesh, in_specs=in_specs, out_specs=out_specs, check_vma=False)
```

```python
import functools

import jax
import jax.numpy as jnp
from jax import lax
from jax.experimental import pallas as pl
from jax.experimental.pallas import tpu as pltpu
from jax.sharding import PartitionSpec as P

STEPS = 8
MOMENTS = 2 * STEPS + 1
ROWS = 16
HALO = 8
MODES = 40
GROUPS = 5
LANES = 128
COLS = 1024
BLOCKS = COLS // LANES
TILES = 64
CHUNKS = (3, 2)

f32 = jnp.float32
bf16 = jnp.bfloat16


def limits(mib):
    return pltpu.CompilerParams(vmem_limit_bytes=mib * 2**20)


def build_left(proj_ref, left_refs, level0):
    lev = lax.axis_index("lev")
    depth = left_refs[0].shape[1]
    pick = (
        lax.broadcasted_iota(jnp.int32, (MODES, 2 * MODES), 1)
        == lax.broadcasted_iota(jnp.int32, (MODES, 2 * MODES), 0) + lev * MODES
    ).astype(bf16)
    own = lax.dot_general(
        pick, proj_ref[...], (((1,), (1,)), ((), ())), preferred_element_type=f32
    ).astype(bf16)
    levels = proj_ref.shape[0]
    spread = (
        lax.broadcasted_iota(jnp.int32, (levels, depth), 0)
        == (lax.broadcasted_iota(jnp.int32, (levels, depth), 1) >> 4) + level0
    ).astype(bf16)
    wide = jnp.dot(own, spread, preferred_element_type=f32)
    row_of = lax.broadcasted_iota(jnp.int32, (8, depth), 1) & (ROWS - 1)
    group = 0
    for ref in left_refs:
        for at in range(0, ref.shape[0], 8 * ROWS):
            part = wide[group * 8:(group + 1) * 8]
            for row in range(0, ROWS, 2):
                two = jnp.concatenate(
                    [jnp.where(row_of == row, part, 0.0), jnp.where(row_of == row + 1, part, 0.0)],
                    axis=0,
                )
                ref[at + row * 8:at + row * 8 + 16, :] = two.astype(bf16)
            group += 1


def own_levels_kernel(proj_ref, inc_ref, *refs):
    lev = lax.axis_index("lev")
    count = proj_ref.shape[0] // 2
    parts = len(CHUNKS)
    acc_refs, other_refs, left_refs = refs[:parts], refs[parts:2 * parts], refs[2 * parts:]

    @pl.when(pl.program_id(0) == 0)
    def _():
        build_left(proj_ref, left_refs, lev * count)
        build_left(proj_ref, other_refs, (1 - lev) * count)

    for acc_ref, left_ref in zip(acc_refs, left_refs):
        acc_ref[...] = jnp.dot(left_ref[...], inc_ref[...], preferred_element_type=f32)


def coded(x):
    t = x * 2.0 ** 13
    square = t * t
    eight = t * 8.0
    y = jnp.where(square < 1.0, eight * jnp.abs(eight), (square * 8.0) * ((square * 8.0) * t))
    return y.astype(bf16)


def decoded(y):
    y = y.astype(f32)
    exponent = jnp.log2(jnp.abs(y)) - 6.0
    root = jnp.exp2(exponent * jnp.where(exponent < 0.0, 0.5, 0.2) - 13.0)
    return jnp.where(y < 0.0, -root, root)


def other_levels_kernel(left_ref, inc_ref, acc_ref, modal_ref, a_ref, b_ref):
    even = (lax.axis_index("tile") & 1) == 0
    modal_ref[...] = acc_ref[...] + jnp.dot(
        left_ref[...], inc_ref[...], preferred_element_type=f32
    )
    half = 8 * HALO
    for at in range(0, a_ref.shape[0], half):
        low = coded(modal_ref[2 * at:2 * at + half, :])
        high = coded(modal_ref[2 * at + half:2 * at + 2 * half, :])
        a_ref[at:at + half, :] = jnp.where(even, high, low)
        b_ref[at:at + half, :] = jnp.where(even, low, high)


def modal_product(increments, projection):
    levels = increments.shape[0]
    depth = levels * ROWS
    flat = increments.reshape(depth, COLS)
    arrived = lax.ppermute(flat, "lev", [(0, 1), (1, 0)])
    width = 256
    grid = (COLS // width,)
    sizes = [groups * 8 * ROWS for groups in CHUNKS]
    column = lambda rows: pl.BlockSpec((rows, width), lambda c: (0, c))
    whole = lambda rows, cols: pl.BlockSpec((rows, cols), lambda c: (0, 0))
    made = pl.pallas_call(
        own_levels_kernel,
        grid=grid,
        in_specs=[whole(2 * levels, 2 * MODES), column(depth)],
        out_specs=[column(n) for n in sizes] + [whole(n, depth) for n in sizes],
        out_shape=[jax.ShapeDtypeStruct((n, COLS), f32) for n in sizes]
        + [jax.ShapeDtypeStruct((n, depth), bf16) for n in sizes],
        scratch_shapes=[pltpu.VMEM((n, depth), bf16) for n in sizes],
        compiler_params=limits(20),
        name="own_levels",
    )(projection.T, flat)
    out = []
    for part, n in enumerate(sizes):
        out.append(pl.pallas_call(
            other_levels_kernel,
            grid=grid,
            in_specs=[whole(n, depth), column(depth), column(n)],
            out_specs=[column(n), column(n // 2), column(n // 2)],
            out_shape=[
                jax.ShapeDtypeStruct((n, COLS), f32),
                jax.ShapeDtypeStruct((n // 2, COLS), bf16),
                jax.ShapeDtypeStruct((n // 2, COLS), bf16),
            ],
            compiler_params=limits(20),
            name="other_levels",
        )(made[len(sizes) + part], arrived, made[part]))
    return out


def is_inner(order, row):
    return order <= row < ROWS - order


INNER_SLOTS, OUTER_SLOTS = {}, {}
for order_ in range(STEPS + 1):
    for row_ in range(ROWS):
        slots_ = INNER_SLOTS if is_inner(order_, row_) else OUTER_SLOTS
        slots_[order_, row_] = len(slots_) * 8
INNER_ROWS, OUTER_ROWS = 8 * len(INNER_SLOTS), 8 * len(OUTER_SLOTS)


def registers(ref, lead, at):
    return [ref[lead, at:at + 8, b * LANES:(b + 1) * LANES] for b in range(BLOCKS)]


def keep(ref, lead, at, values):
    for b, value in enumerate(values):
        ref[lead, at:at + 8, b * LANES:(b + 1) * LANES] = value


class Stencil:
    def __init__(self):
        self.lane = lax.broadcasted_iota(jnp.int32, (8, LANES), 1)
        self.first = self.lane == 0
        self.last = self.lane == LANES - 1

    def beside(self, field):
        right = [pltpu.roll(v, 1, 1) for v in field]
        left = [pltpu.roll(v, LANES - 1, 1) for v in field]
        out = []
        for b in range(BLOCKS):
            lower = jnp.where(self.first, right[b - 1] if b else 0.0, right[b])
            upper = jnp.where(self.last, left[b + 1] if b + 1 < BLOCKS else 0.0, left[b])
            out.append(lower + upper)
        return out

    def next(self, above, here, below, older, factor):
        sides = self.beside(here)
        new = []
        for b in range(BLOCKS):
            value = ((above[b] + below[b]) + sides[b]) * factor
            new.append(value if older is None else value - older[b])
        return new


def total(values):
    while len(values) > 1:
        values = [values[i] + values[i + 1] for i in range(0, len(values), 2)]
    return values[0]


def product(left, right):
    return total([v * w for v, w in zip(left, right)])


def add_moments(moment_ref, sums, lane, group):
    packed = moment_ref[...]
    for index, value in sums.items():
        value = jnp.sum(value, axis=1, keepdims=True)
        packed = packed + jnp.where(lane == index * GROUPS + group, value, 0.0)
    moment_ref[...] = packed


def accumulate(sums, index, value):
    sums[index] = sums[index] + value if index in sums else value


def inner_kernel(*refs):
    modal_refs, (inner_ref, moment_ref) = refs[:-2], refs[-2:]
    step = pl.program_id(0)

    @pl.when(step == 0)
    def _():
        moment_ref[...] = jnp.zeros_like(moment_ref)

    start = 0
    for modal_ref, groups in zip(modal_refs, CHUNKS):
        @pl.when((step >= start) & (step < start + groups))
        def _():
            inner_ref[0, 0:8 * ROWS] = modal_ref[...]
        start += groups
    stencil = Stencil()

    def load(order, row):
        return registers(inner_ref, 0, INNER_SLOTS[order, row])

    sums = {}
    for row in range(ROWS):
        field = load(0, row)
        accumulate(sums, 0, product(field, field))
    for order in range(1, STEPS):
        above, here = load(order - 1, order - 1), load(order - 1, order)
        for row in range(order, ROWS - order):
            below = load(order - 1, row + 1)
            older = None if order == 1 else load(order - 2, row)
            new = stencil.next(above, here, below, older, 0.25 if order == 1 else 0.5)
            keep(inner_ref, 0, INNER_SLOTS[order, row], new)
            accumulate(sums, 2 * order, product(new, new))
            accumulate(sums, 2 * order - 1, product(new, here))
            above, here = here, below
    add_moments(moment_ref, sums, stencil.lane, step)


def inner_basis(modals):
    rows = 8 * ROWS
    starts = [sum(CHUNKS[:c]) for c in range(len(CHUNKS))]
    clamp = lambda s, n: (lambda g: (jnp.clip(g - s, 0, n - 1), 0))
    return pl.pallas_call(
        inner_kernel,
        grid=(GROUPS,),
        in_specs=[pl.BlockSpec((rows, COLS), clamp(s, n)) for s, n in zip(starts, CHUNKS)],
        out_specs=[
            pl.BlockSpec((1, INNER_ROWS, COLS), lambda g: (g, 0, 0)),
            pl.BlockSpec((8, LANES), lambda g: (0, 0)),
        ],
        out_shape=[
            jax.ShapeDtypeStruct((GROUPS, INNER_ROWS, COLS), f32),
            jax.ShapeDtypeStruct((8, LANES), f32),
        ],
        compiler_params=limits(16),
        name="inner",
    )(*modals)


def outer_kernel(start, inner_ref, a_ref, b_ref, known_ref, outer_ref, moment_ref, halo_ref):
    tile = lax.axis_index("tile")
    even = (tile & 1) == 0
    step = pl.program_id(0)

    @pl.when(step == 0)
    def _():
        moment_ref[...] = known_ref[...]

    for row in range(0, HALO, 2):
        part = slice(row * 8, row * 8 + 16)
        a = decoded(a_ref[part, :])
        b = decoded(b_ref[part, :])
        halo_ref[0, part, :] = jnp.where(even, b, a)
        halo_ref[3, part, :] = jnp.where(even, a, b)
    stencil = Stencil()
    half_low = jnp.where(tile == 0, 0.0, 0.5)
    half_high = jnp.where(tile == TILES - 1, 0.0, 0.5)

    def place(order, row):
        if row < 0:
            return halo_ref, order % 3, (row + HALO) * 8
        if row >= ROWS:
            return halo_ref, 3 + order % 3, (row - ROWS) * 8
        if is_inner(order, row):
            return inner_ref, 0, INNER_SLOTS[order, row]
        return outer_ref, 0, OUTER_SLOTS[order, row]

    def load(order, row):
        return registers(*place(order, row))

    sums = {}
    for order in range(1, STEPS + 1):
        for begin, end in ((order - HALO, order), (ROWS - order, ROWS + HALO - order)):
            above, here = load(order - 1, begin - 1), load(order - 1, begin)
            for row in range(begin, end):
                below = load(order - 1, row + 1)
                own = 0 <= row < ROWS
                factor = 0.5 if own else half_low if row < 0 else half_high
                older = None
                if order == 1:
                    factor = factor * 0.5
                else:
                    older = load(order - 2, row)
                new = stencil.next(above, here, below, older, factor)
                keep(*place(order, row), new)
                if own:
                    accumulate(sums, 2 * order, product(new, new))
                    accumulate(sums, 2 * order - 1, product(new, here))
                above, here = here, below
    add_moments(moment_ref, sums, stencil.lane, step + start)


def outer_basis(inner, a, b, known, start, groups):
    halo = 8 * HALO
    return pl.pallas_call(
        functools.partial(outer_kernel, start),
        grid=(groups,),
        in_specs=[
            pl.BlockSpec((1, INNER_ROWS, COLS), lambda g: (g + start, 0, 0)),
            pl.BlockSpec((halo, COLS), lambda g: (g, 0)),
            pl.BlockSpec((halo, COLS), lambda g: (g, 0)),
            pl.BlockSpec((8, LANES), lambda g: (0, 0)),
        ],
        out_specs=[
            pl.BlockSpec((1, OUTER_ROWS, COLS), lambda g: (g, 0, 0)),
            pl.BlockSpec((8, LANES), lambda g: (0, 0)),
        ],
        out_shape=[
            jax.ShapeDtypeStruct((groups, OUTER_ROWS, COLS), f32),
            jax.ShapeDtypeStruct((8, LANES), f32),
        ],
        scratch_shapes=[pltpu.VMEM((6, halo, COLS), f32)],
        compiler_params=limits(16),
        name="outer",
    )(inner, a, b, known)


def coefficients(nu, tau):
    half = 0.5 * tau
    rho = list(nu)
    pi = list(nu)
    one, zero = jnp.ones_like(tau), None
    r = [one]
    p = [one]
    x = [None] * STEPS
    rr = nu[0]

    def plus(a, b):
        if a is None:
            return b
        if b is None:
            return a
        return a + b

    def inner(c, v):
        terms = [ci * vi for ci, vi in zip(c, v)]
        while len(terms) > 1:
            terms = [sum(terms[i:i + 2]) for i in range(0, len(terms), 2)]
        return terms[0]

    for step in range(STEPS):
        top = MOMENTS - 1 - step
        image = []
        for l in range(top):
            near = pi[l + 1] + pi[abs(l - 1)]
            image.append(pi[l] - half * near)
        alpha = rr / inner(p, image)
        x = [plus(x[i], alpha * p[i]) if i < len(p) else x[i] for i in range(STEPS)]
        shifted = [None] * (len(p) + 1)
        for k, value in enumerate(p):
            if k == 0:
                shifted[1] = plus(shifted[1], tau * value)
            else:
                scaled = half * value
                shifted[k + 1] = plus(shifted[k + 1], scaled)
                shifted[k - 1] = plus(shifted[k - 1], scaled)
        moved = []
        for k in range(len(p) + 1):
            own = p[k] if k < len(p) else None
            if shifted[k] is None:
                moved.append(own)
            elif own is None:
                moved.append(-shifted[k])
            else:
                moved.append(own - shifted[k])
        r = [
            (r[k] - alpha * moved[k]) if k < len(r) else -(alpha * moved[k])
            for k in range(len(moved))
        ]
        if step == STEPS - 1:
            break
        rho = [rho[l] - alpha * image[l] for l in range(top)]
        fresh = inner(r, rho)
        beta = fresh / rr
        pi = [rho[l] + beta * pi[l] for l in range(top)]
        p = [plus(r[k], beta * p[k] if k < len(p) else None) for k in range(len(r))]
        rr = fresh
    return x, r


def solve_kernel(sums_ref, helm_ref, inner_ref, *refs):
    outer_refs, (x_ref, r_ref, coef_ref) = refs[:-3], refs[-3:]
    group = pl.program_id(0)

    @pl.when(group == 0)
    def _():
        lane = lax.broadcasted_iota(jnp.int32, (8, LANES), 1)
        sub = lax.broadcasted_iota(jnp.int32, (8, LANES), 0)
        moments = sums_ref[...]
        raw = [moments if k == 0 else pltpu.roll(moments, LANES - GROUPS * k, 1) for k in range(MOMENTS)]
        nu = raw[:2]
        for k in range(2, MOMENTS):
            nu.append(2.0 * raw[k] - nu[k & 1])
        given = jnp.broadcast_to(helm_ref[...], (8, LANES))
        helm = jnp.zeros((8, LANES), f32)
        for g in range(GROUPS):
            value = jnp.sum(jnp.where(lane == sub + 8 * g, given, 0.0), axis=1, keepdims=True)
            helm = jnp.where(lane == g, value, helm)
        x, r = coefficients(nu, 4.0 / (4.0 + helm))
        for g in range(GROUPS):
            for k, value in enumerate(x + r):
                coef_ref[g, k] = jnp.broadcast_to(value[:, g:g + 1], (8, LANES))

    def combine(outer_ref):
        cx = [coef_ref[group, k] for k in range(STEPS)]
        cr = [coef_ref[group, STEPS + k] for k in range(STEPS + 1)]
        for b in range(BLOCKS):
            cols = slice(b * LANES, (b + 1) * LANES)
            for top in range(0, ROWS, 8):
                xs, rs = [], []
                for row in range(top, top + 8):
                    x = r = None
                    for k in range(STEPS + 1):
                        if is_inner(k, row):
                            at = INNER_SLOTS[k, row]
                            field = inner_ref[0, at:at + 8, cols]
                        else:
                            at = OUTER_SLOTS[k, row]
                            field = outer_ref[0, at:at + 8, cols]
                        if k < STEPS:
                            x = cx[k] * field if x is None else x + cx[k] * field
                        r = cr[k] * field if r is None else r + cr[k] * field
                    xs.append(x)
                    rs.append(r)
                x_ref[:, top:top + 8, cols] = jnp.swapaxes(jnp.stack(xs), 0, 1)
                r_ref[:, top:top + 8, cols] = jnp.swapaxes(jnp.stack(rs), 0, 1)

    start = 0
    for outer_ref, groups in zip(outer_refs, CHUNKS):
        pl.when((group >= start) & (group < start + groups))(
            functools.partial(combine, outer_ref)
        )
        start += groups


def solve(sums, helm, inner, outers):
    starts = [sum(CHUNKS[:c]) for c in range(len(CHUNKS))]
    clamp = lambda s, n: (lambda g: (jnp.clip(g - s, 0, n - 1), 0, 0))
    out = jax.ShapeDtypeStruct((MODES, ROWS, COLS), f32)
    return pl.pallas_call(
        solve_kernel,
        grid=(GROUPS,),
        in_specs=[
            pl.BlockSpec((8, LANES), lambda g: (0, 0)),
            pl.BlockSpec((1, LANES), lambda g: (0, 0)),
            pl.BlockSpec((1, INNER_ROWS, COLS), lambda g: (g, 0, 0)),
        ]
        + [pl.BlockSpec((1, OUTER_ROWS, COLS), clamp(s, n)) for s, n in zip(starts, CHUNKS)],
        out_specs=[
            pl.BlockSpec((8, ROWS, COLS), lambda g: (g, 0, 0)),
            pl.BlockSpec((8, ROWS, COLS), lambda g: (g, 0, 0)),
        ],
        out_shape=[out, out],
        scratch_shapes=[pltpu.VMEM((GROUPS, MOMENTS, 8, LANES), f32)],
        compiler_params=limits(16),
        name="solve",
    )(sums, helm, inner, *outers)


def of_everyone(value):
    for mask in (1, 3, 4, 12, 16, 48):
        value = value + lax.ppermute(value, "tile", [(i, i ^ mask) for i in range(TILES)])
    return value


def shards(increments, projection, helmholtz):
    swap_a = [(i, i ^ 1) for i in range(TILES)]
    swap_b = [(i, i + 1) for i in range(1, TILES - 1, 2)]
    swap_b += [(target, source) for source, target in swap_b]
    modals, halos = [], []
    for modal, a, b in modal_product(increments, projection):
        modals.append(modal)
        halos.append((lax.ppermute(a, "tile", swap_a), lax.ppermute(b, "tile", swap_b)))
    inner, moments = inner_basis(modals)
    outers = []
    for part, (a, b) in enumerate(halos):
        outer, moments = outer_basis(inner, a, b, moments, sum(CHUNKS[:part]), CHUNKS[part])
        outers.append(outer)
    helm = jnp.pad(helmholtz[None], ((0, 0), (0, LANES - MODES)))
    return tuple(solve(of_everyone(moments), helm, inner, outers))


def solution(mesh):
    in_specs = (P("lev", "tile", None), P(), P("lev"))
    out_specs = (P("lev", "tile", None), P("lev", "tile", None))
    return jax.shard_map(shards, mesh=mesh, in_specs=in_specs, out_specs=out_specs, check_vma=False)
```

```python
import functools

import jax
import jax.numpy as jnp
from jax import lax
from jax.experimental import pallas as pl
from jax.experimental.pallas import tpu as pltpu
from jax.sharding import PartitionSpec as P

STEPS = 8
MOMENTS = 2 * STEPS + 1
ROWS = 16
HALO = 8
MODES = 40
GROUPS = 5
LANES = 128
COLS = 1024
BLOCKS = COLS // LANES
TILES = 64
CHUNKS = (3, 2)

f32 = jnp.float32
bf16 = jnp.bfloat16


def limits(mib):
    return pltpu.CompilerParams(vmem_limit_bytes=mib * 2**20)


def build_left(proj_ref, left_ref, level0):
    lev = lax.axis_index("lev")
    depth = left_ref.shape[1]
    pick = (
        lax.broadcasted_iota(jnp.int32, (MODES, 2 * MODES), 1)
        == lax.broadcasted_iota(jnp.int32, (MODES, 2 * MODES), 0) + lev * MODES
    ).astype(bf16)
    own = lax.dot_general(
        pick, proj_ref[...], (((1,), (1,)), ((), ())), preferred_element_type=f32
    ).astype(bf16)
    levels = proj_ref.shape[0]
    spread = (
        lax.broadcasted_iota(jnp.int32, (levels, depth), 0)
        == (lax.broadcasted_iota(jnp.int32, (levels, depth), 1) >> 4) + level0
    ).astype(bf16)
    wide = jnp.dot(own, spread, preferred_element_type=f32)
    row_of = lax.broadcasted_iota(jnp.int32, (8, depth), 1) & (ROWS - 1)
    for group in range(GROUPS):
        part = wide[group * 8:(group + 1) * 8]
        for row in range(0, ROWS, 2):
            two = jnp.concatenate(
                [jnp.where(row_of == row, part, 0.0), jnp.where(row_of == row + 1, part, 0.0)],
                axis=0,
            )
            at = group * 8 * ROWS + row * 8
            left_ref[at:at + 16, :] = two.astype(bf16)


def own_levels_kernel(proj_ref, inc_ref, acc_ref, other_left_ref, left_ref):
    lev = lax.axis_index("lev")
    count = proj_ref.shape[0] // 2

    @pl.when(pl.program_id(0) == 0)
    def _():
        build_left(proj_ref, left_ref, lev * count)
        build_left(proj_ref, other_left_ref, (1 - lev) * count)

    acc_ref[...] = jnp.dot(left_ref[...], inc_ref[...], preferred_element_type=f32)


def coded(x):
    t = x * 2.0 ** 13
    square = t * t
    eight = t * 8.0
    y = jnp.where(square < 1.0, eight * jnp.abs(eight), (square * 8.0) * ((square * 8.0) * t))
    return y.astype(bf16)


def decoded(y):
    y = y.astype(f32)
    exponent = jnp.log2(jnp.abs(y)) - 6.0
    root = jnp.exp2(exponent * jnp.where(exponent < 0.0, 0.5, 0.2) - 13.0)
    return jnp.where(y < 0.0, -root, root)


def other_levels_kernel(left_ref, inc_ref, acc_ref, modal_ref, *halo_refs):
    even = (lax.axis_index("tile") & 1) == 0
    modal_ref[...] = acc_ref[...] + jnp.dot(
        left_ref[...], inc_ref[...], preferred_element_type=f32
    )
    half = 8 * HALO
    group = 0
    for a_ref, b_ref in zip(halo_refs[::2], halo_refs[1::2]):
        for at in range(0, a_ref.shape[0], half):
            start = group * 2 * half
            low = coded(modal_ref[start:start + half, :])
            high = coded(modal_ref[start + half:start + 2 * half, :])
            a_ref[at:at + half, :] = jnp.where(even, high, low)
            b_ref[at:at + half, :] = jnp.where(even, low, high)
            group += 1


def modal_product(increments, projection):
    levels = increments.shape[0]
    depth = levels * ROWS
    flat = increments.reshape(depth, COLS)
    arrived = lax.ppermute(flat, "lev", [(0, 1), (1, 0)])
    width = 256
    grid = (COLS // width,)
    count = MODES * ROWS
    column = lambda rows: pl.BlockSpec((rows, width), lambda c: (0, c))
    whole = lambda rows, cols: pl.BlockSpec((rows, cols), lambda c: (0, 0))
    acc, other_left = pl.pallas_call(
        own_levels_kernel,
        grid=grid,
        in_specs=[whole(2 * levels, 2 * MODES), column(depth)],
        out_specs=[column(count), whole(count, depth)],
        out_shape=[
            jax.ShapeDtypeStruct((count, COLS), f32),
            jax.ShapeDtypeStruct((count, depth), bf16),
        ],
        scratch_shapes=[pltpu.VMEM((count, depth), bf16)],
        compiler_params=limits(20),
        name="own_levels",
    )(projection.T, pltpu.with_memory_space_constraint(flat, pltpu.HBM))
    halos = [8 * HALO * n for n in CHUNKS for _ in range(2)]
    modal, *coded_rows = pl.pallas_call(
        other_levels_kernel,
        grid=grid,
        in_specs=[whole(count, depth), column(depth), column(count)],
        out_specs=[column(count)] + [column(n) for n in halos],
        out_shape=[jax.ShapeDtypeStruct((count, COLS), f32)]
        + [jax.ShapeDtypeStruct((n, COLS), bf16) for n in halos],
        compiler_params=limits(20),
        name="other_levels",
    )(other_left, arrived, acc)
    return modal, list(zip(coded_rows[::2], coded_rows[1::2]))


def is_inner(order, row):
    return order <= row < ROWS - order


INNER_SLOTS, OUTER_SLOTS = {}, {}
for order_ in range(STEPS + 1):
    for row_ in range(ROWS):
        slots_ = INNER_SLOTS if is_inner(order_, row_) else OUTER_SLOTS
        slots_[order_, row_] = len(slots_) * 8
INNER_ROWS, OUTER_ROWS = 8 * len(INNER_SLOTS), 8 * len(OUTER_SLOTS)


def registers(ref, lead, at):
    return [ref[lead, at:at + 8, b * LANES:(b + 1) * LANES] for b in range(BLOCKS)]


def keep(ref, lead, at, values):
    for b, value in enumerate(values):
        ref[lead, at:at + 8, b * LANES:(b + 1) * LANES] = value


class Stencil:
    def __init__(self):
        self.lane = lax.broadcasted_iota(jnp.int32, (8, LANES), 1)
        self.first = self.lane == 0
        self.last = self.lane == LANES - 1

    def beside(self, field):
        right = [pltpu.roll(v, 1, 1) for v in field]
        left = [pltpu.roll(v, LANES - 1, 1) for v in field]
        out = []
        for b in range(BLOCKS):
            lower = jnp.where(self.first, right[b - 1] if b else 0.0, right[b])
            upper = jnp.where(self.last, left[b + 1] if b + 1 < BLOCKS else 0.0, left[b])
            out.append(lower + upper)
        return out

    def next(self, above, here, below, older, factor):
        sides = self.beside(here)
        new = []
        for b in range(BLOCKS):
            value = ((above[b] + below[b]) + sides[b]) * factor
            new.append(value if older is None else value - older[b])
        return new


def total(values):
    while len(values) > 1:
        values = [values[i] + values[i + 1] for i in range(0, len(values), 2)]
    return values[0]


def product(left, right):
    return total([v * w for v, w in zip(left, right)])


def add_moments(moment_ref, sums, lane, group):
    packed = moment_ref[...]
    for index, value in sums.items():
        value = jnp.sum(value, axis=1, keepdims=True)
        packed = packed + jnp.where(lane == index * GROUPS + group, value, 0.0)
    moment_ref[...] = packed


def accumulate(sums, index, value):
    sums[index] = sums[index] + value if index in sums else value


def inner_kernel(modal_ref, inner_ref, moment_ref):
    step = pl.program_id(0)

    @pl.when(step == 0)
    def _():
        moment_ref[...] = jnp.zeros_like(moment_ref)

    inner_ref[0, 0:8 * ROWS] = modal_ref[...]
    stencil = Stencil()

    def load(order, row):
        return registers(inner_ref, 0, INNER_SLOTS[order, row])

    sums = {}
    for row in range(ROWS):
        field = load(0, row)
        accumulate(sums, 0, product(field, field))
    for order in range(1, STEPS):
        above, here = load(order - 1, order - 1), load(order - 1, order)
        for row in range(order, ROWS - order):
            below = load(order - 1, row + 1)
            older = None if order == 1 else load(order - 2, row)
            new = stencil.next(above, here, below, older, 0.25 if order == 1 else 0.5)
            keep(inner_ref, 0, INNER_SLOTS[order, row], new)
            accumulate(sums, 2 * order, product(new, new))
            accumulate(sums, 2 * order - 1, product(new, here))
            above, here = here, below
    add_moments(moment_ref, sums, stencil.lane, step)


def inner_basis(modal):
    return pl.pallas_call(
        inner_kernel,
        grid=(GROUPS,),
        in_specs=[pl.BlockSpec((8 * ROWS, COLS), lambda g: (g, 0))],
        out_specs=[
            pl.BlockSpec((1, INNER_ROWS, COLS), lambda g: (g, 0, 0)),
            pl.BlockSpec((8, LANES), lambda g: (0, 0)),
        ],
        out_shape=[
            jax.ShapeDtypeStruct((GROUPS, INNER_ROWS, COLS), f32),
            jax.ShapeDtypeStruct((8, LANES), f32),
        ],
        compiler_params=limits(16),
        name="inner",
    )(modal)


def outer_kernel(start, inner_ref, a_ref, b_ref, known_ref, outer_ref, moment_ref, halo_ref):
    tile = lax.axis_index("tile")
    even = (tile & 1) == 0
    step = pl.program_id(0)

    @pl.when(step == 0)
    def _():
        moment_ref[...] = known_ref[...]

    for row in range(0, HALO, 2):
        part = slice(row * 8, row * 8 + 16)
        a = decoded(a_ref[part, :])
        b = decoded(b_ref[part, :])
        halo_ref[0, part, :] = jnp.where(even, b, a)
        halo_ref[3, part, :] = jnp.where(even, a, b)
    stencil = Stencil()
    half_low = jnp.where(tile == 0, 0.0, 0.5)
    half_high = jnp.where(tile == TILES - 1, 0.0, 0.5)

    def place(order, row):
        if row < 0:
            return halo_ref, order % 3, (row + HALO) * 8
        if row >= ROWS:
            return halo_ref, 3 + order % 3, (row - ROWS) * 8
        if is_inner(order, row):
            return inner_ref, 0, INNER_SLOTS[order, row]
        return outer_ref, 0, OUTER_SLOTS[order, row]

    def load(order, row):
        return registers(*place(order, row))

    sums = {}
    for order in range(1, STEPS + 1):
        for begin, end in ((order - HALO, order), (ROWS - order, ROWS + HALO - order)):
            above, here = load(order - 1, begin - 1), load(order - 1, begin)
            for row in range(begin, end):
                below = load(order - 1, row + 1)
                own = 0 <= row < ROWS
                factor = 0.5 if own else half_low if row < 0 else half_high
                older = None
                if order == 1:
                    factor = factor * 0.5
                else:
                    older = load(order - 2, row)
                new = stencil.next(above, here, below, older, factor)
                keep(*place(order, row), new)
                if own:
                    accumulate(sums, 2 * order, product(new, new))
                    accumulate(sums, 2 * order - 1, product(new, here))
                above, here = here, below
    add_moments(moment_ref, sums, stencil.lane, step + start)


def outer_basis(inner, a, b, known, start, groups):
    halo = 8 * HALO
    return pl.pallas_call(
        functools.partial(outer_kernel, start),
        grid=(groups,),
        in_specs=[
            pl.BlockSpec((1, INNER_ROWS, COLS), lambda g: (g + start, 0, 0)),
            pl.BlockSpec((halo, COLS), lambda g: (g, 0)),
            pl.BlockSpec((halo, COLS), lambda g: (g, 0)),
            pl.BlockSpec((8, LANES), lambda g: (0, 0)),
        ],
        out_specs=[
            pl.BlockSpec((1, OUTER_ROWS, COLS), lambda g: (g, 0, 0)),
            pl.BlockSpec((8, LANES), lambda g: (0, 0)),
        ],
        out_shape=[
            jax.ShapeDtypeStruct((groups, OUTER_ROWS, COLS), f32),
            jax.ShapeDtypeStruct((8, LANES), f32),
        ],
        scratch_shapes=[pltpu.VMEM((6, halo, COLS), f32)],
        compiler_params=limits(16),
        name="outer",
    )(inner, a, b, known)


def coefficients(nu, tau):
    half = 0.5 * tau
    rho = list(nu)
    pi = list(nu)
    one, zero = jnp.ones_like(tau), None
    r = [one]
    p = [one]
    x = [None] * STEPS
    rr = nu[0]

    def plus(a, b):
        if a is None:
            return b
        if b is None:
            return a
        return a + b

    def inner(c, v):
        terms = [ci * vi for ci, vi in zip(c, v)]
        while len(terms) > 1:
            terms = [sum(terms[i:i + 2]) for i in range(0, len(terms), 2)]
        return terms[0]

    for step in range(STEPS):
        top = MOMENTS - 1 - step
        image = []
        for l in range(top):
            near = pi[l + 1] + pi[abs(l - 1)]
            image.append(pi[l] - half * near)
        alpha = rr / inner(p, image)
        x = [plus(x[i], alpha * p[i]) if i < len(p) else x[i] for i in range(STEPS)]
        shifted = [None] * (len(p) + 1)
        for k, value in enumerate(p):
            if k == 0:
                shifted[1] = plus(shifted[1], tau * value)
            else:
                scaled = half * value
                shifted[k + 1] = plus(shifted[k + 1], scaled)
                shifted[k - 1] = plus(shifted[k - 1], scaled)
        moved = []
        for k in range(len(p) + 1):
            own = p[k] if k < len(p) else None
            if shifted[k] is None:
                moved.append(own)
            elif own is None:
                moved.append(-shifted[k])
            else:
                moved.append(own - shifted[k])
        r = [
            (r[k] - alpha * moved[k]) if k < len(r) else -(alpha * moved[k])
            for k in range(len(moved))
        ]
        if step == STEPS - 1:
            break
        rho = [rho[l] - alpha * image[l] for l in range(top)]
        fresh = inner(r, rho)
        beta = fresh / rr
        pi = [rho[l] + beta * pi[l] for l in range(top)]
        p = [plus(r[k], beta * p[k] if k < len(p) else None) for k in range(len(r))]
        rr = fresh
    return x, r


def solve_kernel(sums_ref, helm_ref, inner_ref, *refs):
    outer_refs, (x_ref, r_ref, coef_ref) = refs[:-3], refs[-3:]
    group = pl.program_id(0)

    @pl.when(group == 0)
    def _():
        lane = lax.broadcasted_iota(jnp.int32, (8, LANES), 1)
        sub = lax.broadcasted_iota(jnp.int32, (8, LANES), 0)
        moments = sums_ref[...]
        raw = [moments if k == 0 else pltpu.roll(moments, LANES - GROUPS * k, 1) for k in range(MOMENTS)]
        nu = raw[:2]
        for k in range(2, MOMENTS):
            nu.append(2.0 * raw[k] - nu[k & 1])
        given = jnp.broadcast_to(helm_ref[...], (8, LANES))
        helm = jnp.zeros((8, LANES), f32)
        for g in range(GROUPS):
            value = jnp.sum(jnp.where(lane == sub + 8 * g, given, 0.0), axis=1, keepdims=True)
            helm = jnp.where(lane == g, value, helm)
        x, r = coefficients(nu, 4.0 / (4.0 + helm))
        for g in range(GROUPS):
            for k, value in enumerate(x + r):
                coef_ref[g, k] = jnp.broadcast_to(value[:, g:g + 1], (8, LANES))

    def combine(outer_ref):
        cx = [coef_ref[group, k] for k in range(STEPS)]
        cr = [coef_ref[group, STEPS + k] for k in range(STEPS + 1)]
        for b in range(BLOCKS):
            cols = slice(b * LANES, (b + 1) * LANES)
            for top in range(0, ROWS, 8):
                xs, rs = [], []
                for row in range(top, top + 8):
                    x = r = None
                    for k in range(STEPS + 1):
                        if is_inner(k, row):
                            at = INNER_SLOTS[k, row]
                            field = inner_ref[0, at:at + 8, cols]
                        else:
                            at = OUTER_SLOTS[k, row]
                            field = outer_ref[0, at:at + 8, cols]
                        if k < STEPS:
                            x = cx[k] * field if x is None else x + cx[k] * field
                        r = cr[k] * field if r is None else r + cr[k] * field
                    xs.append(x)
                    rs.append(r)
                x_ref[:, top:top + 8, cols] = jnp.swapaxes(jnp.stack(xs), 0, 1)
                r_ref[:, top:top + 8, cols] = jnp.swapaxes(jnp.stack(rs), 0, 1)

    start = 0
    for outer_ref, groups in zip(outer_refs, CHUNKS):
        pl.when((group >= start) & (group < start + groups))(
            functools.partial(combine, outer_ref)
        )
        start += groups


def solve(sums, helm, inner, outers):
    starts = [sum(CHUNKS[:c]) for c in range(len(CHUNKS))]
    clamp = lambda s, n: (lambda g: (jnp.clip(g - s, 0, n - 1), 0, 0))
    out = jax.ShapeDtypeStruct((MODES, ROWS, COLS), f32)
    return pl.pallas_call(
        solve_kernel,
        grid=(GROUPS,),
        in_specs=[
            pl.BlockSpec((8, LANES), lambda g: (0, 0)),
            pl.BlockSpec((1, LANES), lambda g: (0, 0)),
            pl.BlockSpec((1, INNER_ROWS, COLS), lambda g: (g, 0, 0)),
        ]
        + [pl.BlockSpec((1, OUTER_ROWS, COLS), clamp(s, n)) for s, n in zip(starts, CHUNKS)],
        out_specs=[
            pl.BlockSpec((8, ROWS, COLS), lambda g: (g, 0, 0)),
            pl.BlockSpec((8, ROWS, COLS), lambda g: (g, 0, 0)),
        ],
        out_shape=[out, out],
        scratch_shapes=[pltpu.VMEM((GROUPS, MOMENTS, 8, LANES), f32)],
        compiler_params=limits(16),
        name="solve",
    )(sums, helm, inner, *outers)


def of_everyone(value):
    for stride in (1, 4, 16):
        one, three, two = [
            lax.ppermute(value, "tile", [(i, i ^ (mask * stride)) for i in range(TILES)])
            for mask in (1, 3, 2)
        ]
        value = value + (one + three + two)
    return value


def shards(increments, projection, helmholtz):
    swap_a = [(i, i ^ 1) for i in range(TILES)]
    swap_b = [(i, i + 1) for i in range(1, TILES - 1, 2)]
    swap_b += [(target, source) for source, target in swap_b]
    modal, halos = modal_product(increments, projection)
    halos = [
        (lax.ppermute(a, "tile", swap_a), lax.ppermute(b, "tile", swap_b)) for a, b in halos
    ]
    inner, moments = inner_basis(modal)
    outers = []
    for part, (a, b) in enumerate(halos):
        outer, moments = outer_basis(inner, a, b, moments, sum(CHUNKS[:part]), CHUNKS[part])
        outers.append(outer)
    helm = jnp.pad(helmholtz[None], ((0, 0), (0, LANES - MODES)))
    return tuple(solve(of_everyone(moments), helm, inner, outers))


def solution(mesh):
    in_specs = (P("lev", "tile", None), P(), P("lev"))
    out_specs = (P("lev", "tile", None), P("lev", "tile", None))
    return jax.shard_map(shards, mesh=mesh, in_specs=in_specs, out_specs=out_specs, check_vma=False)
```

```python
import functools

import jax
import jax.numpy as jnp
from jax import lax
from jax.experimental import pallas as pl
from jax.experimental.pallas import tpu as pltpu
from jax.sharding import PartitionSpec as P

STEPS = 8
MOMENTS = 2 * STEPS
ROWS = 16
HALO = 8
MODES = 40
GROUPS = 5
LANES = 128
COLS = 1024
BLOCKS = COLS // LANES
TILES = 64


class ModeSet:
    def __init__(self, *groups):
        self.groups = groups
        self.modes = 8 * len(groups)
        self.base = 8 * groups[0]
        self.segments = LANES // self.modes
        self.length = COLS // self.segments
        self.count = self.length // 8
        self.pitch = self.length + 8

    def rows(self, slabs):
        return slabs * self.pitch + 8


SETS = (ModeSet(0, 1), ModeSet(2, 3), ModeSet(4))
CHUNKS = ((0, 2), (1,))

f32 = jnp.float32
bf16 = jnp.bfloat16


def limits(mib):
    return pltpu.CompilerParams(vmem_limit_bytes=mib * 2**20)


def build_left(proj_ref, left_ref, level0):
    lev = lax.axis_index("lev")
    depth = left_ref.shape[1]
    pick = (
        lax.broadcasted_iota(jnp.int32, (MODES, 2 * MODES), 1)
        == lax.broadcasted_iota(jnp.int32, (MODES, 2 * MODES), 0) + lev * MODES
    ).astype(bf16)
    own = lax.dot_general(
        pick, proj_ref[...], (((1,), (1,)), ((), ())), preferred_element_type=f32
    ).astype(bf16)
    levels = proj_ref.shape[0]
    spread = (
        lax.broadcasted_iota(jnp.int32, (levels, depth), 0)
        == (lax.broadcasted_iota(jnp.int32, (levels, depth), 1) >> 4) + level0
    ).astype(bf16)
    wide = jnp.dot(own, spread, preferred_element_type=f32)
    row_of = lax.broadcasted_iota(jnp.int32, (8, depth), 1) & (ROWS - 1)
    for group in range(GROUPS):
        part = wide[group * 8:(group + 1) * 8]
        for row in range(0, ROWS, 2):
            two = jnp.concatenate(
                [jnp.where(row_of == row, part, 0.0), jnp.where(row_of == row + 1, part, 0.0)],
                axis=0,
            )
            at = group * 8 * ROWS + row * 8
            left_ref[at:at + 16, :] = two.astype(bf16)


def own_levels_kernel(proj_ref, inc_ref, acc_ref, other_left_ref, left_ref):
    lev = lax.axis_index("lev")
    count = proj_ref.shape[0] // 2

    @pl.when(pl.program_id(0) == 0)
    def _():
        build_left(proj_ref, left_ref, lev * count)
        build_left(proj_ref, other_left_ref, (1 - lev) * count)

    acc_ref[...] = jnp.dot(left_ref[...], inc_ref[...], preferred_element_type=f32)


def coded(x):
    t = x * 2.0 ** 13
    square = t * t
    eight = t * 8.0
    y = jnp.where(square < 1.0, eight * jnp.abs(eight), (square * 8.0) * ((square * 8.0) * t))
    return y.astype(bf16)


def decoded(y):
    y = y.astype(f32)
    exponent = jnp.log2(jnp.abs(y)) - 6.0
    root = jnp.exp2(exponent * jnp.where(exponent < 0.0, 0.5, 0.2) - 13.0)
    return jnp.where(y < 0.0, -root, root)


def other_levels_kernel(left_ref, inc_ref, acc_ref, modal_ref):
    modal_ref[...] = acc_ref[...] + jnp.dot(
        left_ref[...], inc_ref[...], preferred_element_type=f32
    )


def modal_product(increments, projection):
    levels = increments.shape[0]
    depth = levels * ROWS
    flat = increments.reshape(depth, COLS)
    arrived = lax.ppermute(flat, "lev", [(0, 1), (1, 0)])
    width = 256
    grid = (COLS // width,)
    count = MODES * ROWS
    column = lambda rows: pl.BlockSpec((rows, width), lambda c: (0, c))
    whole = lambda rows, cols: pl.BlockSpec((rows, cols), lambda c: (0, 0))
    acc, other_left = pl.pallas_call(
        own_levels_kernel,
        grid=grid,
        in_specs=[whole(2 * levels, 2 * MODES), column(depth)],
        out_specs=[column(count), whole(count, depth)],
        out_shape=[
            jax.ShapeDtypeStruct((count, COLS), f32),
            jax.ShapeDtypeStruct((count, depth), bf16),
        ],
        scratch_shapes=[pltpu.VMEM((count, depth), bf16)],
        compiler_params=limits(20),
        name="own_levels",
    )(projection.T, pltpu.with_memory_space_constraint(flat, pltpu.HBM))
    return pl.pallas_call(
        other_levels_kernel,
        grid=grid,
        in_specs=[whole(count, depth), column(depth), column(count)],
        out_specs=column(count),
        out_shape=jax.ShapeDtypeStruct((count, COLS), f32),
        compiler_params=limits(20),
        name="other_levels",
    )(other_left, arrived, acc)


def lanes():
    return lax.broadcasted_iota(jnp.int32, (8, LANES), 1)


def slab_ends(ref, lead, at, kind, first, last):
    after = pltpu.roll(first, LANES - kind.modes, 1)
    after = jnp.where(lanes() >= LANES - kind.modes, 0.0, after)
    before = jnp.where(lanes() < kind.modes, 0.0, pltpu.roll(last, kind.modes, 1))
    end = at + 8 + kind.length
    ref[lead, end:end + 1, :] = after[0:1, :]
    ref[lead, at + 7:at + 8, :] = before[7:8, :]


def slab_store(ref, lead, at, v, value):
    ref[lead, at + 8 + 8 * v:at + 16 + 8 * v, :] = value


def slab_load(ref, lead, at, v, offset=0):
    start = at + 8 + 8 * v + offset
    return ref[lead, start:start + 8, :]


def full(shape):
    return pl.BlockSpec(shape, lambda i: (0,) * len(shape))


def single(kernel, outs, name, mib=16, scratch=()):
    def call(*args):
        return pl.pallas_call(
            kernel,
            grid=(1,),
            in_specs=[full(x.shape) for x in args],
            out_specs=[full(x.shape) for x in outs],
            out_shape=list(outs),
            scratch_shapes=list(scratch),
            compiler_params=limits(mib),
            name=name,
        )(*args)
    return call


def turn_kernel(modal_ref, *refs):
    even = (lax.axis_index("tile") & 1) == 0
    first_refs, halo_refs = refs[:len(SETS)], refs[len(SETS):]
    for part, members in enumerate(CHUNKS):
        a_ref, b_ref = halo_refs[2 * part:2 * part + 2]
        offset = 0
        for member in members:
            kind = SETS[member]

            ref = first_refs[member]

            def columns(row):
                parts = []
                for b in range(BLOCKS):
                    for group in kind.groups:
                        at = (group * ROWS + row) * 8
                        value = modal_ref[at:at + 8, b * LANES:(b + 1) * LANES]
                        parts.append(value)
                        if len(kind.groups) == 1:
                            parts.append(pltpu.roll(value, LANES // 2, 1))
                return jnp.concatenate(parts, axis=0)

            ready = [columns(row) for row in range(4)]
            for row in range(ROWS):
                whole = ready.pop(0).T
                if row + 4 < ROWS:
                    ready.append(columns(row + 4))
                for v in range(kind.count):
                    slab_store(ref, 0, row * kind.pitch, v, whole[8 * v:8 * v + 8])
            for row in range(HALO):
                for v in range(0, kind.count, 2):
                    at = offset + row * kind.length + 8 * v
                    low, high = [
                        coded(jnp.concatenate(
                            [slab_load(ref, 0, start * kind.pitch, v + n) for n in range(2)], axis=0
                        ))
                        for start in (row, row + HALO)
                    ]
                    a_ref[at:at + 16, :] = jnp.where(even, high, low)
                    b_ref[at:at + 16, :] = jnp.where(even, low, high)
            for row in range(ROWS):
                at = row * kind.pitch
                slab_ends(
                    ref, 0, at, kind, slab_load(ref, 0, at, 0), slab_load(ref, 0, at, kind.count - 1)
                )
            offset += HALO * kind.length


def turn(modal):
    firsts = [jax.ShapeDtypeStruct((1, kind.rows(ROWS), LANES), f32) for kind in SETS]
    halos = [
        jax.ShapeDtypeStruct((sum(HALO * SETS[m].length for m in members), LANES), bf16)
        for members in CHUNKS for _ in range(2)
    ]
    out = single(turn_kernel, firsts + halos, "turn")(modal)
    halos = out[len(SETS):]
    return out[:len(SETS)], list(zip(halos[::2], halos[1::2]))


def is_inner(order, row):
    return order <= row < ROWS - order


INNER_SLOTS, OUTER_SLOTS = {}, {}
for order_ in range(1, STEPS + 1):
    for row_ in range(ROWS):
        slots_ = INNER_SLOTS if is_inner(order_, row_) else OUTER_SLOTS
        slots_[order_, row_] = len(slots_)
STRIP = 8


def sweep(kind, order, begin, end, place, sums, factor_of):
    for strip in range(0, kind.count, STRIP):
        span = range(strip, strip + STRIP)
        near = lambda row: [slab_load(*place(order - 1, row), v) for v in span]
        above, here = near(begin - 1), near(begin)
        for row in range(begin, end):
            below = near(row + 1)
            factor = factor_of(row)
            squares, crosses = [], []
            for n, v in enumerate(span):
                left = slab_load(*place(order - 1, row), v, -1)
                right = slab_load(*place(order - 1, row), v, 1)
                value = ((above[n] + below[n]) + (left + right)) * factor
                if order > 1:
                    value = value - slab_load(*place(order - 2, row), v)
                ref, lead, at = place(order, row)
                slab_store(ref, lead, at, v, value)
                if v == kind.count - 1:
                    slab_ends(ref, lead, at, kind, slab_load(ref, lead, at, 0), value)
                squares.append(value * value)
                crosses.append(value * here[n])
            if 0 <= row < ROWS:
                if 2 * order < MOMENTS:
                    accumulate(sums, 2 * order, total(squares))
                accumulate(sums, 2 * order - 1, total(crosses))
            above, here = here, below


def total(values):
    while len(values) > 1:
        values = [values[i] + values[i + 1] for i in range(0, len(values), 2)]
    return values[0]


def accumulate(sums, index, value):
    sums[index] = sums[index] + value if index in sums else value


def inner_kernel(*refs):
    count = len(SETS)
    for kind, first_ref, inner_ref, moment_ref in zip(
        SETS, refs[:count], refs[count:2 * count], refs[2 * count:]
    ):
        def place(order, row):
            if order == 0:
                return first_ref, 0, row * kind.pitch
            return inner_ref, 0, INNER_SLOTS[order, row] * kind.pitch

        sums = {}
        for row in range(ROWS):
            values = [slab_load(*place(0, row), v) for v in range(kind.count)]
            accumulate(sums, 0, total([v * v for v in values]))
        for order in range(1, STEPS):
            factor = 0.25 if order == 1 else 0.5
            sweep(kind, order, order, ROWS - order, place, sums, lambda row: factor)
        for index in range(MOMENTS):
            if index in sums:
                moment_ref[index:index + 1, :] = jnp.sum(sums[index], axis=0, keepdims=True)
            else:
                moment_ref[index:index + 1, :] = jnp.zeros((1, LANES), f32)


def inner_basis(firsts):
    outs = [jax.ShapeDtypeStruct((1, kind.rows(len(INNER_SLOTS)), LANES), f32) for kind in SETS]
    outs += [jax.ShapeDtypeStruct((MOMENTS, LANES), f32)] * len(SETS)
    out = single(inner_kernel, outs, "inner")(*firsts)
    return out[:len(SETS)], out[len(SETS):]


def outer_kernel(members, a_ref, b_ref, known_ref, *refs):
    count = len(members)
    ins, (outs, (moment_ref, *halo_refs)) = refs[:3 * count], (
        refs[3 * count:4 * count], refs[4 * count:]
    )
    tile = lax.axis_index("tile")
    even = (tile & 1) == 0
    half_low = jnp.where(tile == 0, 0.0, 0.5)
    half_high = jnp.where(tile == TILES - 1, 0.0, 0.5)
    lane = lax.broadcasted_iota(jnp.int32, (MOMENTS, LANES), 1)
    moments = known_ref[...]
    offset = 0
    for n, member in enumerate(members):
        kind = SETS[member]
        first_ref, inner_ref, part_ref = ins[3 * n:3 * n + 3]
        outer_ref, halo_ref = outs[n], halo_refs[n]
        for row in range(HALO):
            for v in range(0, kind.count, 2):
                at = offset + row * kind.length + 8 * v
                a = decoded(a_ref[at:at + 16, :])
                b = decoded(b_ref[at:at + 16, :])
                for side, both in ((0, jnp.where(even, b, a)), (3, jnp.where(even, a, b))):
                    slab_store(halo_ref, side, row * kind.pitch, v, both[:8])
                    slab_store(halo_ref, side, row * kind.pitch, v + 1, both[8:])
                    if v == 0:
                        first = {} if side == 0 else first
                        first[side] = both[:8]
                    if v + 2 == kind.count:
                        slab_ends(halo_ref, side, row * kind.pitch, kind, first[side], both[8:])
        offset += HALO * kind.length

        def place(order, row):
            if row < 0:
                return halo_ref, order % 3, (row + HALO) * kind.pitch
            if row >= ROWS:
                return halo_ref, 3 + order % 3, (row - ROWS) * kind.pitch
            if order == 0:
                return first_ref, 0, row * kind.pitch
            if is_inner(order, row):
                return inner_ref, 0, INNER_SLOTS[order, row] * kind.pitch
            return outer_ref, 0, OUTER_SLOTS[order, row] * kind.pitch

        sums = {}
        for order in range(1, STEPS + 1):
            def factor_of(row):
                half = 0.5 if 0 <= row < ROWS else half_low if row < 0 else half_high
                return half * 0.5 if order == 1 else half

            for begin, end in ((order - HALO, order), (ROWS - order, ROWS + HALO - order)):
                sweep(kind, order, begin, end, place, sums, factor_of)
        rows = [
            jnp.sum(sums[i], axis=0, keepdims=True) if i in sums else jnp.zeros((1, LANES), f32)
            for i in range(MOMENTS)
        ]
        part = part_ref[...] + jnp.concatenate(rows, axis=0)
        step = LANES // 2
        while step >= kind.modes:
            part = part + pltpu.roll(part, step, 1)
            step //= 2
        mine = (lane >= kind.base) & (lane < kind.base + kind.modes)
        moments = moments + jnp.where(mine, part, 0.0)
    moment_ref[...] = moments


def outer_basis(members, halo, known, firsts, inners, parts):
    outs = [
        jax.ShapeDtypeStruct((1, SETS[m].rows(len(OUTER_SLOTS)), LANES), f32) for m in members
    ]
    outs += [jax.ShapeDtypeStruct((MOMENTS, LANES), f32)]
    args = [x for m in members for x in (firsts[m], inners[m], parts[m])]
    scratch = [pltpu.VMEM((6, SETS[m].rows(HALO), LANES), f32) for m in members]
    out = single(functools.partial(outer_kernel, members), outs, "outer", 24, scratch)(
        *halo, known, *args
    )
    return out[:-1], out[-1]


def coefficients(nu, tau):
    half = 0.5 * tau
    rho = list(nu)
    pi = list(nu)
    one, zero = jnp.ones_like(tau), None
    r = [one]
    p = [one]
    x = [None] * STEPS
    rr = nu[0]

    def plus(a, b):
        if a is None:
            return b
        if b is None:
            return a
        return a + b

    def inner(c, v):
        terms = [ci * vi for ci, vi in zip(c, v)]
        while len(terms) > 1:
            terms = [sum(terms[i:i + 2]) for i in range(0, len(terms), 2)]
        return terms[0]

    for step in range(STEPS):
        top = MOMENTS - 1 - step
        image = []
        for l in range(top):
            near = pi[l + 1] + pi[abs(l - 1)]
            image.append(pi[l] - half * near)
        alpha = rr / inner(p, image)
        x = [plus(x[i], alpha * p[i]) if i < len(p) else x[i] for i in range(STEPS)]
        shifted = [None] * (len(p) + 1)
        for k, value in enumerate(p):
            if k == 0:
                shifted[1] = plus(shifted[1], tau * value)
            else:
                scaled = half * value
                shifted[k + 1] = plus(shifted[k + 1], scaled)
                shifted[k - 1] = plus(shifted[k - 1], scaled)
        moved = []
        for k in range(len(p) + 1):
            own = p[k] if k < len(p) else None
            if shifted[k] is None:
                moved.append(own)
            elif own is None:
                moved.append(-shifted[k])
            else:
                moved.append(own - shifted[k])
        r = [
            (r[k] - alpha * moved[k]) if k < len(r) else -(alpha * moved[k])
            for k in range(len(moved))
        ]
        if step == STEPS - 1:
            break
        rho = [rho[l] - alpha * image[l] for l in range(top)]
        fresh = inner(r, rho)
        beta = fresh / rr
        pi = [rho[l] + beta * pi[l] for l in range(top)]
        p = [plus(r[k], beta * p[k] if k < len(p) else None) for k in range(len(r))]
        rr = fresh
    return x, r


def solve_kernel(sums_ref, helm_ref, *refs):
    count = len(SETS)
    fields = [refs[3 * n:3 * n + 3] for n in range(count)]
    x_out, r_out, x_ref, r_ref, stage_ref, coef_ref, sems = refs[3 * count:]
    raw = [sums_ref[k:k + 1, :] for k in range(MOMENTS)]
    nu = raw[:2]
    for k in range(2, MOMENTS):
        nu.append(2.0 * raw[k] - nu[k & 1])
    x, r = coefficients(nu, 4.0 / (4.0 + helm_ref[...]))
    for k, value in enumerate(x + r):
        coef_ref[k:k + 1, :] = value
    coefs = coef_ref[...]
    lane_all = lax.broadcasted_iota(jnp.int32, coefs.shape, 1)
    low_half = lanes() < LANES // 2
    copies = []
    for kind, (first_ref, inner_ref, outer_ref) in zip(SETS, fields):
        mine = (lane_all >= kind.base) & (lane_all < kind.base + kind.modes)
        own = jnp.where(mine, coefs, 0.0)
        step = kind.modes
        while step < LANES:
            own = own + pltpu.roll(own, step, 1)
            step *= 2
        spread = [jnp.broadcast_to(own[k:k + 1, :], (8, LANES)) for k in range(2 * STEPS + 1)]
        cx, cr = spread[:STEPS], spread[STEPS:]

        def combined(row):
            xs, rs = [], []
            for v in range(kind.count):
                x = r = None
                for k in range(STEPS + 1):
                    if k == 0:
                        field = slab_load(first_ref, 0, row * kind.pitch, v)
                    elif is_inner(k, row):
                        field = slab_load(inner_ref, 0, INNER_SLOTS[k, row] * kind.pitch, v)
                    else:
                        field = slab_load(outer_ref, 0, OUTER_SLOTS[k, row] * kind.pitch, v)
                    if k < STEPS:
                        x = cx[k] * field if x is None else x + cx[k] * field
                    r = cr[k] * field if r is None else r + cr[k] * field
                xs.append(x)
                rs.append(r)
            return xs, rs

        for top in range(0, ROWS, 8):
            if len(kind.groups) == 2:
                for row in range(8):
                    for which, values in enumerate(combined(top + row)):
                        stage_ref[which, row] = jnp.concatenate(values, axis=0).T
            else:
                for row in range(0, 8, 2):
                    for which, (one, two) in enumerate(
                        zip(combined(top + row), combined(top + row + 1))
                    ):
                        both = jnp.concatenate(one + two, axis=0).T
                        for b in range(BLOCKS):
                            even = both[16 * b:16 * b + 8]
                            odd = both[16 * b + 8:16 * b + 16]
                            half = LANES // 2
                            stage_ref[which, row, 8 * b:8 * b + 8, :] = jnp.where(
                                low_half, even, pltpu.roll(odd, half, 1)
                            )
                            stage_ref[which, row + 1, 8 * b:8 * b + 8, :] = jnp.where(
                                low_half, pltpu.roll(even, half, 1), odd
                            )
            for which, ref in enumerate((x_ref, r_ref)):
                for b in range(BLOCKS):
                    for n, group in enumerate(kind.groups):
                        at = (b * len(kind.groups) + n) * 8
                        block = jnp.swapaxes(stage_ref[which, :, at:at + 8, :], 0, 1)
                        ref[8 * group:8 * group + 8, top:top + 8, b * LANES:(b + 1) * LANES] = block
        for ref, out in ((x_ref, x_out), (r_ref, r_out)):
            part = pl.ds(kind.base, kind.modes)
            copy = pltpu.make_async_copy(ref.at[part], out.at[part], sems.at[len(copies)])
            copy.start()
            copies.append(copy)
    for copy in copies:
        copy.wait()


def solve(sums, helm, firsts, inners, outers):
    out = jax.ShapeDtypeStruct((MODES, ROWS, COLS), f32)
    args = [sums, helm] + [x for trio in zip(firsts, inners, outers) for x in trio]
    return pl.pallas_call(
        solve_kernel,
        grid=(1,),
        in_specs=[full(x.shape) for x in args],
        out_specs=[pl.BlockSpec(memory_space=pl.ANY)] * 2,
        out_shape=[out, out],
        scratch_shapes=[
            pltpu.VMEM((MODES, ROWS, COLS), f32),
            pltpu.VMEM((MODES, ROWS, COLS), f32),
            pltpu.VMEM((2, 8, LANES, LANES), f32),
            pltpu.VMEM((24, LANES), f32),
            pltpu.SemaphoreType.DMA((2 * len(SETS),)),
        ],
        compiler_params=limits(16),
        name="solve",
    )(*args)


def of_everyone(value):
    for stride in (1, 4, 16):
        one, three, two = [
            lax.ppermute(value, "tile", [(i, i ^ (mask * stride)) for i in range(TILES)])
            for mask in (1, 3, 2)
        ]
        value = value + (one + three + two)
    return value


def shards(increments, projection, helmholtz):
    swap_a = [(i, i ^ 1) for i in range(TILES)]
    swap_b = [(i, i + 1) for i in range(1, TILES - 1, 2)]
    swap_b += [(target, source) for source, target in swap_b]
    firsts, halos = turn(modal_product(increments, projection))
    halos = [
        (lax.ppermute(a, "tile", swap_a), lax.ppermute(b, "tile", swap_b)) for a, b in halos
    ]
    inners, parts = inner_basis(firsts)
    moments = jnp.zeros((MOMENTS, LANES), f32)
    outers = {}
    for members, halo in zip(CHUNKS, halos):
        made, moments = outer_basis(members, halo, moments, firsts, inners, parts)
        outers.update(zip(members, made))
    helm = jnp.pad(helmholtz[None], ((0, 0), (0, LANES - MODES)))
    outers = [outers[n] for n in range(len(SETS))]
    return tuple(solve(of_everyone(moments), helm, firsts, inners, outers))


def solution(mesh):
    in_specs = (P("lev", "tile", None), P(), P("lev"))
    out_specs = (P("lev", "tile", None), P("lev", "tile", None))
    return jax.shard_map(shards, mesh=mesh, in_specs=in_specs, out_specs=out_specs, check_vma=False)
```

```python
import functools

import jax
import jax.numpy as jnp
from jax import lax
from jax.experimental import pallas as pl
from jax.experimental.pallas import tpu as pltpu
from jax.sharding import PartitionSpec as P

STEPS = 8
MOMENTS = 2 * STEPS
ROWS = 16
HALO = 8
MODES = 40
GROUPS = 5
LANES = 128
COLS = 1024
BLOCKS = COLS // LANES
TILES = 64


class ModeSet:
    def __init__(self, *groups):
        self.groups = groups
        self.modes = 8 * len(groups)
        self.base = 8 * groups[0]
        self.segments = LANES // self.modes
        self.length = COLS // self.segments
        self.count = self.length // 8
        self.pitch = self.length + 8

    def rows(self, slabs):
        return slabs * self.pitch + 8


SETS = (ModeSet(0, 1), ModeSet(2, 3), ModeSet(4))
CHUNKS = ((0, 2), (1,))

f32 = jnp.float32
bf16 = jnp.bfloat16


def limits(mib):
    return pltpu.CompilerParams(vmem_limit_bytes=mib * 2**20)


def spread_projection(proj_ref, level0, depth):
    lev = lax.axis_index("lev")
    pick = (
        lax.broadcasted_iota(jnp.int32, (MODES, 2 * MODES), 1)
        == lax.broadcasted_iota(jnp.int32, (MODES, 2 * MODES), 0) + lev * MODES
    ).astype(bf16)
    own = lax.dot_general(
        pick, proj_ref[...], (((1,), (1,)), ((), ())), preferred_element_type=f32
    ).astype(bf16)
    levels = proj_ref.shape[0]
    spread = (
        lax.broadcasted_iota(jnp.int32, (levels, depth), 0)
        == (lax.broadcasted_iota(jnp.int32, (levels, depth), 1) >> 4) + level0
    ).astype(bf16)
    return jnp.dot(own, spread, preferred_element_type=f32)


def build_left(wide, left_refs):
    row_of = lax.broadcasted_iota(jnp.int32, (8, wide.shape[1]), 1) & (ROWS - 1)
    for members, ref in zip(CHUNKS, left_refs):
        at = 0
        for group in groups_of(members):
            part = wide[group * 8:(group + 1) * 8]
            for row in range(0, ROWS, 2):
                two = jnp.concatenate(
                    [jnp.where(row_of == row, part, 0.0), jnp.where(row_of == row + 1, part, 0.0)],
                    axis=0,
                )
                ref[at:at + 16, :] = two.astype(bf16)
                at += 16


def groups_of(members):
    return [group for member in members for group in SETS[member].groups]


def own_levels_kernel(proj_ref, inc_ref, *refs):
    lev = lax.axis_index("lev")
    count = proj_ref.shape[0] // 2
    parts = len(CHUNKS)
    acc_refs, other_refs, left_refs = refs[:parts], refs[parts:2 * parts], refs[2 * parts:]
    depth = left_refs[0].shape[1]

    @pl.when(pl.program_id(0) == 0)
    def _():
        build_left(spread_projection(proj_ref, lev * count, depth), left_refs)

    @pl.when(pl.program_id(0) == pl.num_programs(0) - 1)
    def _():
        build_left(spread_projection(proj_ref, (1 - lev) * count, depth), other_refs)
        for acc_ref, left_ref in zip(acc_refs, left_refs):
            acc_ref[...] = jnp.dot(left_ref[...], inc_ref[...], preferred_element_type=f32)

    @pl.when(pl.program_id(0) < pl.num_programs(0) - 1)
    def _():
        for acc_ref, left_ref in zip(acc_refs, left_refs):
            acc_ref[...] = jnp.dot(left_ref[...], inc_ref[...], preferred_element_type=f32)


def coded(x):
    t = x * 2.0 ** 13
    square = t * t
    eight = t * 8.0
    y = jnp.where(square < 1.0, eight * jnp.abs(eight), (square * 8.0) * ((square * 8.0) * t))
    return y.astype(bf16)


def decoded(y):
    y = y.astype(f32)
    exponent = jnp.log2(jnp.abs(y)) - 6.0
    root = jnp.exp2(exponent * jnp.where(exponent < 0.0, 0.5, 0.2) - 13.0)
    return jnp.where(y < 0.0, -root, root)


def other_levels_kernel(left_ref, inc_ref, acc_ref, modal_ref):
    modal_ref[...] = acc_ref[...] + jnp.dot(
        left_ref[...], inc_ref[...], preferred_element_type=f32
    )


def modal_product(increments, projection):
    levels = increments.shape[0]
    depth = levels * ROWS
    flat = increments.reshape(depth, COLS)
    arrived = lax.ppermute(flat, "lev", [(0, 1), (1, 0)])
    width = 256
    grid = (COLS // width,)
    sizes = [8 * ROWS * len(groups_of(members)) for members in CHUNKS]
    column = lambda rows: pl.BlockSpec((rows, width), lambda c: (0, c))
    whole = lambda rows, cols: pl.BlockSpec((rows, cols), lambda c: (0, 0))
    in_hbm = lambda x: pltpu.with_memory_space_constraint(x, pltpu.HBM)
    made = pl.pallas_call(
        own_levels_kernel,
        grid=grid,
        in_specs=[whole(2 * levels, 2 * MODES), column(depth)],
        out_specs=[column(n) for n in sizes] + [whole(n, depth) for n in sizes],
        out_shape=[jax.ShapeDtypeStruct((n, COLS), f32) for n in sizes]
        + [jax.ShapeDtypeStruct((n, depth), bf16) for n in sizes],
        scratch_shapes=[pltpu.VMEM((n, depth), bf16) for n in sizes],
        compiler_params=limits(20),
        name="own_levels",
    )(in_hbm(projection.T), in_hbm(flat))
    return [
        pl.pallas_call(
            other_levels_kernel,
            grid=grid,
            in_specs=[whole(n, depth), column(depth), column(n)],
            out_specs=column(n),
            out_shape=jax.ShapeDtypeStruct((n, COLS), f32),
            compiler_params=limits(20),
            name="other_levels",
        )(made[len(sizes) + part], arrived, made[part])
        for part, n in enumerate(sizes)
    ]


def lanes():
    return lax.broadcasted_iota(jnp.int32, (8, LANES), 1)


def slab_ends(ref, lead, at, kind, first, last):
    after = pltpu.roll(first, LANES - kind.modes, 1)
    after = jnp.where(lanes() >= LANES - kind.modes, 0.0, after)
    before = jnp.where(lanes() < kind.modes, 0.0, pltpu.roll(last, kind.modes, 1))
    end = at + 8 + kind.length
    ref[lead, end:end + 1, :] = after[0:1, :]
    ref[lead, at + 7:at + 8, :] = before[7:8, :]


def slab_store(ref, lead, at, v, value):
    start = at + 8 + 8 * v
    ref[lead, start:start + value.shape[0], :] = value


def slab_load(ref, lead, at, v, offset=0, count=1):
    start = at + 8 + 8 * v + offset
    if offset == 0 or count == 1:
        return ref[lead, start:start + 8 * count, :]
    parts = [ref[lead, start + 8 * n:start + 8 * n + 8, :] for n in range(count)]
    return jnp.concatenate(parts, axis=0)


def full(shape):
    return pl.BlockSpec(shape, lambda i: (0,) * len(shape))


def single(kernel, outs, name, mib=16, scratch=()):
    def call(*args):
        return pl.pallas_call(
            kernel,
            grid=(1,),
            in_specs=[full(x.shape) for x in args],
            out_specs=[full(x.shape) for x in outs],
            out_shape=list(outs),
            scratch_shapes=list(scratch),
            compiler_params=limits(mib),
            name=name,
        )(*args)
    return call


def turn_kernel(members, modal_ref, *refs):
    even = (lax.axis_index("tile") & 1) == 0
    first_refs, (a_ref, b_ref) = refs[:len(members)], refs[len(members):]
    places = {group: n for n, group in enumerate(groups_of(members))}
    offset = 0
    for n, member in enumerate(members):
        kind = SETS[member]
        ref = first_refs[n]

        def columns(row):
            parts = []
            for b in range(BLOCKS):
                for group in kind.groups:
                    at = (places[group] * ROWS + row) * 8
                    value = modal_ref[at:at + 8, b * LANES:(b + 1) * LANES]
                    parts.append(value)
                    if len(kind.groups) == 1:
                        parts.append(pltpu.roll(value, LANES // 2, 1))
            return jnp.concatenate(parts, axis=0)

        ready = [columns(row) for row in range(4)]
        for row in range(ROWS):
            whole = ready.pop(0).T
            if row + 4 < ROWS:
                ready.append(columns(row + 4))
            slab_store(ref, 0, row * kind.pitch, 0, whole[:kind.length])
        for row in range(HALO):
            at = offset + row * kind.length
            low, high = [
                coded(slab_load(ref, 0, start * kind.pitch, 0, 0, kind.count))
                for start in (row, row + HALO)
            ]
            a_ref[at:at + kind.length, :] = jnp.where(even, high, low)
            b_ref[at:at + kind.length, :] = jnp.where(even, low, high)
        for row in range(ROWS):
            at = row * kind.pitch
            slab_ends(
                ref, 0, at, kind, slab_load(ref, 0, at, 0), slab_load(ref, 0, at, kind.count - 1)
            )
        offset += HALO * kind.length


def turn(members, modal):
    outs = [jax.ShapeDtypeStruct((1, SETS[m].rows(ROWS), LANES), f32) for m in members]
    edge = sum(HALO * SETS[m].length for m in members)
    outs += [jax.ShapeDtypeStruct((edge, LANES), bf16)] * 2
    out = single(functools.partial(turn_kernel, members), outs, "turn")(modal)
    return out[:-2], out[-2:]


def is_inner(order, row):
    return order <= row < ROWS - order


INNER_SLOTS, OUTER_SLOTS = {}, {}
for order_ in range(1, STEPS + 1):
    for row_ in range(ROWS):
        slots_ = INNER_SLOTS if is_inner(order_, row_) else OUTER_SLOTS
        slots_[order_, row_] = len(slots_)
STRIP = 8


def sweep(kind, order, begin, end, place, sums, factor_of):
    for strip in range(0, kind.count, STRIP):
        near = lambda row: slab_load(*place(order - 1, row), strip, 0, STRIP)
        above, here = near(begin - 1), near(begin)
        for row in range(begin, end):
            below = near(row + 1)
            left = slab_load(*place(order - 1, row), strip, -1, STRIP)
            right = slab_load(*place(order - 1, row), strip, 1, STRIP)
            value = ((above + below) + (left + right)) * factor_of(row)
            if order > 1:
                value = value - slab_load(*place(order - 2, row), strip, 0, STRIP)
            ref, lead, at = place(order, row)
            slab_store(ref, lead, at, strip, value)
            if strip + STRIP == kind.count:
                slab_ends(ref, lead, at, kind, slab_load(ref, lead, at, 0), value[-8:])
            if 0 <= row < ROWS:
                if 2 * order < MOMENTS:
                    accumulate(sums, 2 * order, total(value * value))
                accumulate(sums, 2 * order - 1, total(value * here))
            above, here = here, below


def total(values):
    parts = [values[at:at + 8] for at in range(0, values.shape[0], 8)]
    while len(parts) > 1:
        parts = [parts[i] + parts[i + 1] for i in range(0, len(parts), 2)]
    return parts[0]


def accumulate(sums, index, value):
    sums[index] = sums[index] + value if index in sums else value


def inner_kernel(*refs):
    count = len(SETS)
    for kind, first_ref, inner_ref, moment_ref in zip(
        SETS, refs[:count], refs[count:2 * count], refs[2 * count:]
    ):
        def place(order, row):
            if order == 0:
                return first_ref, 0, row * kind.pitch
            return inner_ref, 0, INNER_SLOTS[order, row] * kind.pitch

        sums = {}
        for row in range(ROWS):
            values = slab_load(*place(0, row), 0, 0, kind.count)
            accumulate(sums, 0, total(values * values))
        for order in range(1, STEPS):
            factor = 0.25 if order == 1 else 0.5
            sweep(kind, order, order, ROWS - order, place, sums, lambda row: factor)
        for index in range(MOMENTS):
            if index in sums:
                moment_ref[index:index + 1, :] = jnp.sum(sums[index], axis=0, keepdims=True)
            else:
                moment_ref[index:index + 1, :] = jnp.zeros((1, LANES), f32)


def inner_basis(firsts):
    outs = [jax.ShapeDtypeStruct((1, kind.rows(len(INNER_SLOTS)), LANES), f32) for kind in SETS]
    outs += [jax.ShapeDtypeStruct((MOMENTS, LANES), f32)] * len(SETS)
    out = single(inner_kernel, outs, "inner")(*firsts)
    return out[:len(SETS)], out[len(SETS):]


def outer_kernel(members, a_ref, b_ref, known_ref, *refs):
    count = len(members)
    ins, (outs, (moment_ref, *halo_refs)) = refs[:3 * count], (
        refs[3 * count:4 * count], refs[4 * count:]
    )
    tile = lax.axis_index("tile")
    even = (tile & 1) == 0
    half_low = jnp.where(tile == 0, 0.0, 0.5)
    half_high = jnp.where(tile == TILES - 1, 0.0, 0.5)
    lane = lax.broadcasted_iota(jnp.int32, (MOMENTS, LANES), 1)
    moments = known_ref[...]
    offset = 0
    for n, member in enumerate(members):
        kind = SETS[member]
        first_ref, inner_ref, part_ref = ins[3 * n:3 * n + 3]
        outer_ref, halo_ref = outs[n], halo_refs[n]
        for row in range(HALO):
            at = offset + row * kind.length
            a = decoded(a_ref[at:at + kind.length, :])
            b = decoded(b_ref[at:at + kind.length, :])
            for side, value in ((0, jnp.where(even, b, a)), (3, jnp.where(even, a, b))):
                slab_store(halo_ref, side, row * kind.pitch, 0, value)
                slab_ends(halo_ref, side, row * kind.pitch, kind, value[:8], value[-8:])
        offset += HALO * kind.length

        def place(order, row):
            if row < 0:
                return halo_ref, order % 3, (row + HALO) * kind.pitch
            if row >= ROWS:
                return halo_ref, 3 + order % 3, (row - ROWS) * kind.pitch
            if order == 0:
                return first_ref, 0, row * kind.pitch
            if is_inner(order, row):
                return inner_ref, 0, INNER_SLOTS[order, row] * kind.pitch
            return outer_ref, 0, OUTER_SLOTS[order, row] * kind.pitch

        sums = {}
        for order in range(1, STEPS + 1):
            def factor_of(row):
                half = 0.5 if 0 <= row < ROWS else half_low if row < 0 else half_high
                return half * 0.5 if order == 1 else half

            for begin, end in ((order - HALO, order), (ROWS - order, ROWS + HALO - order)):
                sweep(kind, order, begin, end, place, sums, factor_of)
        rows = [
            jnp.sum(sums[i], axis=0, keepdims=True) if i in sums else jnp.zeros((1, LANES), f32)
            for i in range(MOMENTS)
        ]
        part = part_ref[...] + jnp.concatenate(rows, axis=0)
        step = LANES // 2
        while step >= kind.modes:
            part = part + pltpu.roll(part, step, 1)
            step //= 2
        mine = (lane >= kind.base) & (lane < kind.base + kind.modes)
        moments = moments + jnp.where(mine, part, 0.0)
    moment_ref[...] = moments


def outer_basis(members, halo, known, firsts, inners, parts):
    outs = [
        jax.ShapeDtypeStruct((1, SETS[m].rows(len(OUTER_SLOTS)), LANES), f32) for m in members
    ]
    outs += [jax.ShapeDtypeStruct((MOMENTS, LANES), f32)]
    args = [x for m in members for x in (firsts[m], inners[m], parts[m])]
    scratch = [pltpu.VMEM((6, SETS[m].rows(HALO), LANES), f32) for m in members]
    out = single(functools.partial(outer_kernel, members), outs, "outer", 24, scratch)(
        *halo, known, *args
    )
    return out[:-1], out[-1]


def coefficients(nu, tau):
    half = 0.5 * tau
    rho = list(nu)
    pi = list(nu)
    one, zero = jnp.ones_like(tau), None
    r = [one]
    p = [one]
    x = [None] * STEPS
    rr = nu[0]

    def plus(a, b):
        if a is None:
            return b
        if b is None:
            return a
        return a + b

    def inner(c, v):
        terms = [ci * vi for ci, vi in zip(c, v)]
        while len(terms) > 1:
            terms = [sum(terms[i:i + 2]) for i in range(0, len(terms), 2)]
        return terms[0]

    for step in range(STEPS):
        top = MOMENTS - 1 - step
        image = []
        for l in range(top):
            near = pi[l + 1] + pi[abs(l - 1)]
            image.append(pi[l] - half * near)
        alpha = rr / inner(p, image)
        x = [plus(x[i], alpha * p[i]) if i < len(p) else x[i] for i in range(STEPS)]
        shifted = [None] * (len(p) + 1)
        for k, value in enumerate(p):
            if k == 0:
                shifted[1] = plus(shifted[1], tau * value)
            else:
                scaled = half * value
                shifted[k + 1] = plus(shifted[k + 1], scaled)
                shifted[k - 1] = plus(shifted[k - 1], scaled)
        moved = []
        for k in range(len(p) + 1):
            own = p[k] if k < len(p) else None
            if shifted[k] is None:
                moved.append(own)
            elif own is None:
                moved.append(-shifted[k])
            else:
                moved.append(own - shifted[k])
        r = [
            (r[k] - alpha * moved[k]) if k < len(r) else -(alpha * moved[k])
            for k in range(len(moved))
        ]
        if step == STEPS - 1:
            break
        rho = [rho[l] - alpha * image[l] for l in range(top)]
        fresh = inner(r, rho)
        beta = fresh / rr
        pi = [rho[l] + beta * pi[l] for l in range(top)]
        p = [plus(r[k], beta * p[k] if k < len(p) else None) for k in range(len(r))]
        rr = fresh
    return x, r


def solve_kernel(sums_ref, helm_ref, *refs):
    count = len(SETS)
    fields = [refs[3 * n:3 * n + 3] for n in range(count)]
    x_out, r_out, x_ref, r_ref, stage_ref, coef_ref, sems = refs[3 * count:]
    raw = [sums_ref[k:k + 1, :] for k in range(MOMENTS)]
    nu = raw[:2]
    for k in range(2, MOMENTS):
        nu.append(2.0 * raw[k] - nu[k & 1])
    x, r = coefficients(nu, 4.0 / (4.0 + helm_ref[...]))
    for k, value in enumerate(x + r):
        coef_ref[k:k + 1, :] = value
    coefs = coef_ref[...]
    lane_all = lax.broadcasted_iota(jnp.int32, coefs.shape, 1)
    low_half = lanes() < LANES // 2
    copies = []
    for kind, (first_ref, inner_ref, outer_ref) in zip(SETS, fields):
        mine = (lane_all >= kind.base) & (lane_all < kind.base + kind.modes)
        own = jnp.where(mine, coefs, 0.0)
        step = kind.modes
        while step < LANES:
            own = own + pltpu.roll(own, step, 1)
            step *= 2
        spread = [jnp.broadcast_to(own[k:k + 1, :], (8, LANES))[None] for k in range(2 * STEPS + 1)]
        cx, cr = spread[:STEPS], spread[STEPS:]

        def combined(row):
            xs, rs = [], []
            for strip in range(0, kind.count, STRIP):
                x = r = None
                for k in range(STEPS + 1):
                    if k == 0:
                        ref, slot = first_ref, row
                    elif is_inner(k, row):
                        ref, slot = inner_ref, INNER_SLOTS[k, row]
                    else:
                        ref, slot = outer_ref, OUTER_SLOTS[k, row]
                    field = slab_load(ref, 0, slot * kind.pitch, strip, 0, STRIP)
                    field = field.reshape(STRIP, 8, LANES)
                    if k < STEPS:
                        x = cx[k] * field if x is None else x + cx[k] * field
                    r = cr[k] * field if r is None else r + cr[k] * field
                xs.append(x.reshape(STRIP * 8, LANES))
                rs.append(r.reshape(STRIP * 8, LANES))
            return jnp.concatenate(xs, axis=0), jnp.concatenate(rs, axis=0)

        for top in range(0, ROWS, 8):
            if len(kind.groups) == 2:
                for row in range(8):
                    for which, values in enumerate(combined(top + row)):
                        stage_ref[which, row] = values.T
            else:
                for row in range(0, 8, 2):
                    for which, (one, two) in enumerate(
                        zip(combined(top + row), combined(top + row + 1))
                    ):
                        both = jnp.concatenate([one, two], axis=0).T
                        for b in range(BLOCKS):
                            even = both[16 * b:16 * b + 8]
                            odd = both[16 * b + 8:16 * b + 16]
                            half = LANES // 2
                            stage_ref[which, row, 8 * b:8 * b + 8, :] = jnp.where(
                                low_half, even, pltpu.roll(odd, half, 1)
                            )
                            stage_ref[which, row + 1, 8 * b:8 * b + 8, :] = jnp.where(
                                low_half, pltpu.roll(even, half, 1), odd
                            )
            for which, ref in enumerate((x_ref, r_ref)):
                for b in range(BLOCKS):
                    for n, group in enumerate(kind.groups):
                        at = (b * len(kind.groups) + n) * 8
                        block = jnp.swapaxes(stage_ref[which, :, at:at + 8, :], 0, 1)
                        ref[8 * group:8 * group + 8, top:top + 8, b * LANES:(b + 1) * LANES] = block
        for ref, out in ((x_ref, x_out), (r_ref, r_out)):
            part = pl.ds(kind.base, kind.modes)
            copy = pltpu.make_async_copy(ref.at[part], out.at[part], sems.at[len(copies)])
            copy.start()
            copies.append(copy)
    for copy in copies:
        copy.wait()


def solve(sums, helm, firsts, inners, outers):
    out = jax.ShapeDtypeStruct((MODES, ROWS, COLS), f32)
    args = [sums, helm] + [x for trio in zip(firsts, inners, outers) for x in trio]
    return pl.pallas_call(
        solve_kernel,
        grid=(1,),
        in_specs=[full(x.shape) for x in args],
        out_specs=[pl.BlockSpec(memory_space=pl.ANY)] * 2,
        out_shape=[out, out],
        scratch_shapes=[
            pltpu.VMEM((MODES, ROWS, COLS), f32),
            pltpu.VMEM((MODES, ROWS, COLS), f32),
            pltpu.VMEM((2, 8, LANES, LANES), f32),
            pltpu.VMEM((24, LANES), f32),
            pltpu.SemaphoreType.DMA((2 * len(SETS),)),
        ],
        compiler_params=limits(16),
        name="solve",
    )(*args)


def of_everyone(value):
    for stride in (1, 4, 16):
        one, three, two = [
            lax.ppermute(value, "tile", [(i, i ^ (mask * stride)) for i in range(TILES)])
            for mask in (1, 3, 2)
        ]
        value = value + (one + three + two)
    return value


def shards(increments, projection, helmholtz):
    swap_a = [(i, i ^ 1) for i in range(TILES)]
    swap_b = [(i, i + 1) for i in range(1, TILES - 1, 2)]
    swap_b += [(target, source) for source, target in swap_b]
    firsts, halos = {}, []
    for members, modal in zip(CHUNKS, modal_product(increments, projection)):
        made, (a, b) = turn(members, modal)
        firsts.update(zip(members, made))
        a = lax.ppermute(a, "tile", swap_a)
        halos.append((a, lax.ppermute(b, "tile", swap_b)))
    firsts = [firsts[n] for n in range(len(SETS))]
    inners, parts = inner_basis(firsts)
    moments = jnp.zeros((MOMENTS, LANES), f32)
    outers = {}
    for members, halo in zip(CHUNKS, halos):
        made, moments = outer_basis(members, halo, moments, firsts, inners, parts)
        outers.update(zip(members, made))
    helm = jnp.pad(helmholtz[None], ((0, 0), (0, LANES - MODES)))
    outers = [outers[n] for n in range(len(SETS))]
    return tuple(solve(of_everyone(moments), helm, firsts, inners, outers))


def solution(mesh):
    in_specs = (P("lev", "tile", None), P(), P("lev"))
    out_specs = (P("lev", "tile", None), P("lev", "tile", None))
    return jax.shard_map(shards, mesh=mesh, in_specs=in_specs, out_specs=out_specs, check_vma=False)
```

```python
import functools

import jax
import jax.numpy as jnp
from jax import lax
from jax.experimental import pallas as pl
from jax.experimental.pallas import tpu as pltpu
from jax.sharding import PartitionSpec as P


STEPS = 8
MOMENTS = 2 * STEPS
ROWS = 16
HALO = 8
MODES = 40
LANES = 128
COLS = 1024
BLOCKS = COLS // LANES
TILES = 64


class ModeSet:
    def __init__(self, *groups):
        self.groups = groups
        self.modes = 8 * len(groups)
        self.base = 8 * groups[0]
        self.segments = LANES // self.modes
        self.length = COLS // self.segments
        self.count = self.length // 8
        self.pitch = self.length + 8

    def rows(self, slabs):
        return slabs * self.pitch + 8


SETS = (ModeSet(0, 1), ModeSet(2, 3), ModeSet(4))
CHUNKS = ((0, 2), (1,))

f32 = jnp.float32
bf16 = jnp.bfloat16


def limits(mib):
    return pltpu.CompilerParams(vmem_limit_bytes=mib * 2**20)


def spread_projection(proj_ref, level0, depth):
    lev = lax.axis_index("lev")
    pick = (
        lax.broadcasted_iota(jnp.int32, (MODES, 2 * MODES), 1)
        == lax.broadcasted_iota(jnp.int32, (MODES, 2 * MODES), 0) + lev * MODES
    ).astype(bf16)
    own = lax.dot_general(
        pick, proj_ref[...], (((1,), (1,)), ((), ())), preferred_element_type=f32
    ).astype(bf16)
    levels = proj_ref.shape[0]
    spread = (
        lax.broadcasted_iota(jnp.int32, (levels, depth), 0)
        == (lax.broadcasted_iota(jnp.int32, (levels, depth), 1) >> 4) + level0
    ).astype(bf16)
    return jnp.dot(own, spread, preferred_element_type=f32)


def build_left(wide, left_refs):
    row_of = lax.broadcasted_iota(jnp.int32, (8, wide.shape[1]), 1) & (ROWS - 1)
    for members, ref in zip(CHUNKS, left_refs):
        at = 0
        for group in groups_of(members):
            part = wide[group * 8:(group + 1) * 8]
            for row in range(0, ROWS, 2):
                two = jnp.concatenate(
                    [jnp.where(row_of == row, part, 0.0), jnp.where(row_of == row + 1, part, 0.0)],
                    axis=0,
                )
                ref[at:at + 16, :] = two.astype(bf16)
                at += 16


def groups_of(members):
    return [group for member in members for group in SETS[member].groups]


def own_levels_kernel(proj_ref, inc_ref, *refs):
    lev = lax.axis_index("lev")
    count = proj_ref.shape[0] // 2
    parts = len(CHUNKS)
    acc_refs, other_refs, left_refs = refs[:parts], refs[parts:2 * parts], refs[2 * parts:]
    depth = left_refs[0].shape[1]

    @pl.when(pl.program_id(0) == 0)
    def _():
        build_left(spread_projection(proj_ref, lev * count, depth), left_refs)

    @pl.when(pl.program_id(0) == pl.num_programs(0) - 1)
    def _():
        build_left(spread_projection(proj_ref, (1 - lev) * count, depth), other_refs)
        for acc_ref, left_ref in zip(acc_refs, left_refs):
            acc_ref[...] = jnp.dot(left_ref[...], inc_ref[...], preferred_element_type=f32)

    @pl.when(pl.program_id(0) < pl.num_programs(0) - 1)
    def _():
        for acc_ref, left_ref in zip(acc_refs, left_refs):
            acc_ref[...] = jnp.dot(left_ref[...], inc_ref[...], preferred_element_type=f32)


def coded(x):
    t = x * 2.0 ** 13
    square = t * t
    eight = t * 8.0
    y = jnp.where(square < 1.0, eight * jnp.abs(eight), (square * 8.0) * ((square * 8.0) * t))
    return y.astype(bf16)


def decoded(y):
    y = y.astype(f32)
    exponent = jnp.log2(jnp.abs(y)) - 6.0
    root = jnp.exp2(exponent * jnp.where(exponent < 0.0, 0.5, 0.2) - 13.0)
    return jnp.where(y < 0.0, -root, root)


def other_levels_kernel(left_ref, inc_ref, acc_ref, modal_ref):
    modal_ref[...] = acc_ref[...] + jnp.dot(
        left_ref[...], inc_ref[...], preferred_element_type=f32
    )


def modal_product(increments, projection):
    levels = increments.shape[0]
    depth = levels * ROWS
    flat = increments.reshape(depth, COLS)
    arrived = lax.ppermute(flat, "lev", [(0, 1), (1, 0)])
    width = 256
    grid = (COLS // width,)
    sizes = [8 * ROWS * len(groups_of(members)) for members in CHUNKS]
    column = lambda rows: pl.BlockSpec((rows, width), lambda c: (0, c))
    whole = lambda rows, cols: pl.BlockSpec((rows, cols), lambda c: (0, 0))
    in_hbm = lambda x: pltpu.with_memory_space_constraint(x, pltpu.HBM)
    made = pl.pallas_call(
        own_levels_kernel,
        grid=grid,
        in_specs=[whole(2 * levels, 2 * MODES), column(depth)],
        out_specs=[column(n) for n in sizes] + [whole(n, depth) for n in sizes],
        out_shape=[jax.ShapeDtypeStruct((n, COLS), f32) for n in sizes]
        + [jax.ShapeDtypeStruct((n, depth), bf16) for n in sizes],
        scratch_shapes=[pltpu.VMEM((n, depth), bf16) for n in sizes],
        compiler_params=limits(20),
        name="own_levels",
    )(in_hbm(projection.T), in_hbm(flat))
    return [
        pl.pallas_call(
            other_levels_kernel,
            grid=grid,
            in_specs=[whole(n, depth), column(depth), column(n)],
            out_specs=column(n),
            out_shape=jax.ShapeDtypeStruct((n, COLS), f32),
            compiler_params=limits(20),
            name="other_levels",
        )(made[len(sizes) + part], arrived, made[part])
        for part, n in enumerate(sizes)
    ]


def lanes():
    return lax.broadcasted_iota(jnp.int32, (8, LANES), 1)


def slab_ends(ref, lead, at, kind, first, last):
    after = pltpu.roll(first, LANES - kind.modes, 1)
    after = jnp.where(lanes() >= LANES - kind.modes, 0.0, after)
    before = jnp.where(lanes() < kind.modes, 0.0, pltpu.roll(last, kind.modes, 1))
    end = at + 8 + kind.length
    ref[lead, end:end + 1, :] = after[0:1, :]
    ref[lead, at + 7:at + 8, :] = before[7:8, :]


def slab_store(ref, lead, at, v, value):
    start = at + 8 + 8 * v
    ref[lead, start:start + value.shape[0], :] = value


def slab_load(ref, lead, at, v, offset=0, count=1):
    start = at + 8 + 8 * v + offset
    if offset == 0 or count == 1:
        return ref[lead, start:start + 8 * count, :]
    parts = [ref[lead, start + 8 * n:start + 8 * n + 8, :] for n in range(count)]
    return jnp.concatenate(parts, axis=0)


def full(shape):
    return pl.BlockSpec(shape, lambda i: (0,) * len(shape))


def single(kernel, outs, mib=16, scratch=()):
    def call(*args):
        return pl.pallas_call(
            kernel,
            grid=(1,),
            in_specs=[full(x.shape) for x in args],
            out_specs=[full(x.shape) for x in outs],
            out_shape=list(outs),
            scratch_shapes=list(scratch),
            compiler_params=limits(mib),
        )(*args)

    return call


def turn_kernel(members, modal_ref, *refs):
    even = (lax.axis_index("tile") & 1) == 0
    first_refs, (a_ref, b_ref) = refs[:len(members)], refs[len(members):]
    places = {group: n for n, group in enumerate(groups_of(members))}
    offset = 0
    for n, member in enumerate(members):
        kind = SETS[member]
        ref = first_refs[n]

        def columns(row):
            parts = []
            for b in range(BLOCKS):
                for group in kind.groups:
                    at = (places[group] * ROWS + row) * 8
                    value = modal_ref[at:at + 8, b * LANES:(b + 1) * LANES]
                    parts.append(value)
                    if len(kind.groups) == 1:
                        parts.append(pltpu.roll(value, LANES // 2, 1))
            return jnp.concatenate(parts, axis=0)

        ready = [columns(row) for row in range(4)]
        for row in range(ROWS):
            whole = ready.pop(0).T
            if row + 4 < ROWS:
                ready.append(columns(row + 4))
            slab_store(ref, 0, row * kind.pitch, 0, whole[:kind.length])
        for row in range(HALO):
            at = offset + row * kind.length
            low, high = [
                coded(slab_load(ref, 0, start * kind.pitch, 0, 0, kind.count))
                for start in (row, row + HALO)
            ]
            a_ref[at:at + kind.length, :] = jnp.where(even, high, low)
            b_ref[at:at + kind.length, :] = jnp.where(even, low, high)
        for row in range(ROWS):
            at = row * kind.pitch
            slab_ends(
                ref, 0, at, kind, slab_load(ref, 0, at, 0), slab_load(ref, 0, at, kind.count - 1)
            )
        offset += HALO * kind.length


def turn(members, modal):
    outs = [jax.ShapeDtypeStruct((1, SETS[m].rows(ROWS), LANES), f32) for m in members]
    edge = sum(HALO * SETS[m].length for m in members)
    outs += [jax.ShapeDtypeStruct((edge, LANES), bf16)] * 2
    out = single(functools.partial(turn_kernel, members), outs)(modal)
    return out[:-2], out[-2:]


def is_inner(order, row):
    return order <= row < ROWS - order


INNER_SLOTS, OUTER_SLOTS = {}, {}
for order_ in range(1, STEPS + 1):
    for row_ in range(ROWS):
        slots_ = INNER_SLOTS if is_inner(order_, row_) else OUTER_SLOTS
        slots_[order_, row_] = len(slots_)
STRIP = 4


def sweep(kind, order, begin, end, place, sums, factor_of):
    for strip in range(0, kind.count, STRIP):
        near = lambda row: slab_load(*place(order - 1, row), strip, 0, STRIP)
        above, here = near(begin - 1), near(begin)
        for row in range(begin, end):
            below = near(row + 1)
            left = slab_load(*place(order - 1, row), strip, -1, STRIP)
            right = slab_load(*place(order - 1, row), strip, 1, STRIP)
            value = ((above + below) + (left + right)) * factor_of(row)
            if order > 1:
                value = value - slab_load(*place(order - 2, row), strip, 0, STRIP)
            ref, lead, at = place(order, row)
            slab_store(ref, lead, at, strip, value)
            if strip + STRIP == kind.count:
                slab_ends(ref, lead, at, kind, slab_load(ref, lead, at, 0), value[-8:])
            if 0 <= row < ROWS:
                if 2 * order < MOMENTS:
                    accumulate(sums, 2 * order, total(value * value))
                accumulate(sums, 2 * order - 1, total(value * here))
            above, here = here, below


def total(values):
    parts = [values[at:at + 8] for at in range(0, values.shape[0], 8)]
    while len(parts) > 1:
        parts = [parts[i] + parts[i + 1] for i in range(0, len(parts), 2)]
    return parts[0]


def accumulate(sums, index, value):
    sums[index] = sums[index] + value if index in sums else value


def inner_kernel(*refs):
    count = len(SETS)
    for kind, first_ref, inner_ref, moment_ref in zip(
        SETS, refs[:count], refs[count:2 * count], refs[2 * count:]
    ):
        def place(order, row):
            if order == 0:
                return first_ref, 0, row * kind.pitch
            return inner_ref, 0, INNER_SLOTS[order, row] * kind.pitch

        sums = {}
        for row in range(ROWS):
            values = slab_load(*place(0, row), 0, 0, kind.count)
            accumulate(sums, 0, total(values * values))
        for order in range(1, STEPS):
            factor = 0.25 if order == 1 else 0.5
            sweep(kind, order, order, ROWS - order, place, sums, lambda row: factor)
        for index in range(MOMENTS):
            if index in sums:
                moment_ref[index:index + 1, :] = jnp.sum(sums[index], axis=0, keepdims=True)
            else:
                moment_ref[index:index + 1, :] = jnp.zeros((1, LANES), f32)


def inner_basis(firsts):
    outs = [jax.ShapeDtypeStruct((1, kind.rows(len(INNER_SLOTS)), LANES), f32) for kind in SETS]
    outs += [jax.ShapeDtypeStruct((MOMENTS, LANES), f32)] * len(SETS)
    out = single(inner_kernel, outs)(*firsts)
    return out[:len(SETS)], out[len(SETS):]


def outer_kernel(members, a_ref, b_ref, known_ref, *refs):
    count = len(members)
    ins, (outs, (moment_ref, *halo_refs)) = refs[:3 * count], (
        refs[3 * count:4 * count], refs[4 * count:]
    )
    tile = lax.axis_index("tile")
    even = (tile & 1) == 0
    half_low = jnp.where(tile == 0, 0.0, 0.5)
    half_high = jnp.where(tile == TILES - 1, 0.0, 0.5)
    lane = lax.broadcasted_iota(jnp.int32, (MOMENTS, LANES), 1)
    moments = known_ref[...]
    offset = 0
    for n, member in enumerate(members):
        kind = SETS[member]
        first_ref, inner_ref, part_ref = ins[3 * n:3 * n + 3]
        outer_ref, halo_ref = outs[n], halo_refs[n]
        for row in range(HALO):
            at = offset + row * kind.length
            a = decoded(a_ref[at:at + kind.length, :])
            b = decoded(b_ref[at:at + kind.length, :])
            for side, value in ((0, jnp.where(even, b, a)), (3, jnp.where(even, a, b))):
                slab_store(halo_ref, side, row * kind.pitch, 0, value)
                slab_ends(halo_ref, side, row * kind.pitch, kind, value[:8], value[-8:])
        offset += HALO * kind.length

        def place(order, row):
            if row < 0:
                return halo_ref, order % 3, (row + HALO) * kind.pitch
            if row >= ROWS:
                return halo_ref, 3 + order % 3, (row - ROWS) * kind.pitch
            if order == 0:
                return first_ref, 0, row * kind.pitch
            if is_inner(order, row):
                return inner_ref, 0, INNER_SLOTS[order, row] * kind.pitch
            return outer_ref, 0, OUTER_SLOTS[order, row] * kind.pitch

        sums = {}
        for order in range(1, STEPS + 1):
            def factor_of(row):
                half = 0.5 if 0 <= row < ROWS else half_low if row < 0 else half_high
                return half * 0.5 if order == 1 else half

            for begin, end in ((order - HALO, order), (ROWS - order, ROWS + HALO - order)):
                sweep(kind, order, begin, end, place, sums, factor_of)
        rows = [
            jnp.sum(sums[i], axis=0, keepdims=True) if i in sums else jnp.zeros((1, LANES), f32)
            for i in range(MOMENTS)
        ]
        part = part_ref[...] + jnp.concatenate(rows, axis=0)
        step = LANES // 2
        while step >= kind.modes:
            part = part + pltpu.roll(part, step, 1)
            step //= 2
        mine = (lane >= kind.base) & (lane < kind.base + kind.modes)
        moments = moments + jnp.where(mine, part, 0.0)
    moment_ref[...] = moments


def outer_basis(members, halo, known, firsts, inners, parts):
    outs = [
        jax.ShapeDtypeStruct((1, SETS[m].rows(len(OUTER_SLOTS)), LANES), f32) for m in members
    ]
    outs += [jax.ShapeDtypeStruct((MOMENTS, LANES), f32)]
    args = [x for m in members for x in (firsts[m], inners[m], parts[m])]
    scratch = [pltpu.VMEM((6, SETS[m].rows(HALO), LANES), f32) for m in members]
    out = single(functools.partial(outer_kernel, members), outs, 24, scratch)(*halo, known, *args)
    return out[:-1], out[-1]


def coefficients(nu, tau):
    half = 0.5 * tau
    rho = list(nu)
    pi = list(nu)
    one = jnp.ones_like(tau)
    r = [one]
    p = [one]
    x = [None] * STEPS
    rr = nu[0]

    def plus(a, b):
        if a is None:
            return b
        if b is None:
            return a
        return a + b

    def inner(c, v):
        terms = [ci * vi for ci, vi in zip(c, v)]
        while len(terms) > 1:
            terms = [sum(terms[i:i + 2]) for i in range(0, len(terms), 2)]
        return terms[0]

    for step in range(STEPS):
        top = MOMENTS - 1 - step
        image = []
        for l in range(top):
            near = pi[l + 1] + pi[abs(l - 1)]
            image.append(pi[l] - half * near)
        alpha = rr / inner(p, image)
        x = [plus(x[i], alpha * p[i]) if i < len(p) else x[i] for i in range(STEPS)]
        shifted = [None] * (len(p) + 1)
        for k, value in enumerate(p):
            if k == 0:
                shifted[1] = plus(shifted[1], tau * value)
            else:
                scaled = half * value
                shifted[k + 1] = plus(shifted[k + 1], scaled)
                shifted[k - 1] = plus(shifted[k - 1], scaled)
        moved = []
        for k in range(len(p) + 1):
            own = p[k] if k < len(p) else None
            if shifted[k] is None:
                moved.append(own)
            elif own is None:
                moved.append(-shifted[k])
            else:
                moved.append(own - shifted[k])
        r = [
            (r[k] - alpha * moved[k]) if k < len(r) else -(alpha * moved[k])
            for k in range(len(moved))
        ]
        if step == STEPS - 1:
            break
        rho = [rho[l] - alpha * image[l] for l in range(top)]
        fresh = inner(r, rho)
        beta = fresh / rr
        pi = [rho[l] + beta * pi[l] for l in range(top)]
        p = [plus(r[k], beta * p[k] if k < len(p) else None) for k in range(len(r))]
        rr = fresh
    return x, r


def solve_kernel(sums_ref, helm_ref, *refs):
    count = len(SETS)
    fields = [refs[3 * n:3 * n + 3] for n in range(count)]
    x_out, r_out, x_ref, r_ref, mix_ref, stage_ref, coef_ref, sems = refs[3 * count:]
    raw = [sums_ref[k:k + 1, :] for k in range(MOMENTS)]
    nu = raw[:2]
    for k in range(2, MOMENTS):
        nu.append(2.0 * raw[k] - nu[k & 1])
    x, r = coefficients(nu, 4.0 / (4.0 + helm_ref[...]))
    for k, value in enumerate(x + r):
        coef_ref[k:k + 1, :] = value
    coefs = coef_ref[...]
    lane_all = lax.broadcasted_iota(jnp.int32, coefs.shape, 1)
    low_half = lanes() < LANES // 2
    copies = []
    for kind, (first_ref, inner_ref, outer_ref) in zip(SETS, fields):
        mine = (lane_all >= kind.base) & (lane_all < kind.base + kind.modes)
        own = jnp.where(mine, coefs, 0.0)
        step = kind.modes
        while step < LANES:
            own = own + pltpu.roll(own, step, 1)
            step *= 2
        spread = [jnp.broadcast_to(own[k:k + 1, :], (8, LANES))[None] for k in range(2 * STEPS + 1)]
        cx, cr = spread[:STEPS], spread[STEPS:]

        def combine(row, at):
            for strip in range(0, kind.count, STRIP):
                x = r = None
                for k in range(STEPS + 1):
                    if k == 0:
                        ref, slot = first_ref, row
                    elif is_inner(k, row):
                        ref, slot = inner_ref, INNER_SLOTS[k, row]
                    else:
                        ref, slot = outer_ref, OUTER_SLOTS[k, row]
                    field = slab_load(ref, 0, slot * kind.pitch, strip, 0, STRIP)
                    field = field.reshape(STRIP, 8, LANES)
                    if k < STEPS:
                        x = cx[k] * field if x is None else x + cx[k] * field
                    r = cr[k] * field if r is None else r + cr[k] * field
                for which, value in ((0, x), (1, r)):
                    start = at + 8 * strip
                    mix_ref[which, start:start + 8 * STRIP, :] = value.reshape(8 * STRIP, LANES)

        for top in range(0, ROWS, 8):
            for row in range(8):
                combine(top + row, row * kind.length)
            step = LANES // kind.length
            for row in range(0, 8, step):
                start = row * kind.length
                for which in range(2):
                    both = mix_ref[which, start:start + LANES, :].T
                    if step == 1:
                        stage_ref[which, row] = both
                        continue
                    for b in range(BLOCKS):
                        even = both[16 * b:16 * b + 8]
                        odd = both[16 * b + 8:16 * b + 16]
                        half = LANES // 2
                        stage_ref[which, row, 8 * b:8 * b + 8, :] = jnp.where(
                            low_half, even, pltpu.roll(odd, half, 1)
                        )
                        stage_ref[which, row + 1, 8 * b:8 * b + 8, :] = jnp.where(
                            low_half, pltpu.roll(even, half, 1), odd
                        )
            for which, ref in enumerate((x_ref, r_ref)):
                for b in range(BLOCKS):
                    for n, group in enumerate(kind.groups):
                        at = (b * len(kind.groups) + n) * 8
                        block = jnp.swapaxes(stage_ref[which, :, at:at + 8, :], 0, 1)
                        ref[8 * group:8 * group + 8, top:top + 8, b * LANES:(b + 1) * LANES] = block
        for ref, out in ((x_ref, x_out), (r_ref, r_out)):
            part = pl.ds(kind.base, kind.modes)
            copy = pltpu.make_async_copy(ref.at[part], out.at[part], sems.at[len(copies)])
            copy.start()
            copies.append(copy)
    for copy in copies:
        copy.wait()


def solve(sums, helm, firsts, inners, outers):
    out = jax.ShapeDtypeStruct((MODES, ROWS, COLS), f32)
    args = [sums, helm] + [x for trio in zip(firsts, inners, outers) for x in trio]
    return pl.pallas_call(
        solve_kernel,
        grid=(1,),
        in_specs=[full(x.shape) for x in args],
        out_specs=[pl.BlockSpec(memory_space=pl.ANY)] * 2,
        out_shape=[out, out],
        scratch_shapes=[
            pltpu.VMEM((MODES, ROWS, COLS), f32),
            pltpu.VMEM((MODES, ROWS, COLS), f32),
            pltpu.VMEM((2, 8 * LANES, LANES), f32),
            pltpu.VMEM((2, 8, LANES, LANES), f32),
            pltpu.VMEM((24, LANES), f32),
            pltpu.SemaphoreType.DMA((2 * len(SETS),)),
        ],
        compiler_params=limits(16),
        name="solve",
    )(*args)


def of_everyone(value):
    for stride in (1, 4, 16):
        one, three, two = [
            lax.ppermute(value, "tile", [(i, i ^ (mask * stride)) for i in range(TILES)])
            for mask in (1, 3, 2)
        ]
        value = value + (one + three + two)
    return value


def shards(increments, projection, helmholtz):
    swap_a = [(i, i ^ 1) for i in range(TILES)]
    swap_b = [(i, i + 1) for i in range(1, TILES - 1, 2)]
    swap_b += [(target, source) for source, target in swap_b]
    firsts, halos = {}, []
    for members, modal in zip(CHUNKS, modal_product(increments, projection)):
        made, (a, b) = turn(members, modal)
        firsts.update(zip(members, made))
        a = lax.ppermute(a, "tile", swap_a)
        b = lax.ppermute(b, "tile", swap_b)
        halos.append((a, b))
    firsts = [firsts[n] for n in range(len(SETS))]
    inners, parts = inner_basis(firsts)
    moments = jnp.zeros((MOMENTS, LANES), f32)
    outers = {}
    for members, halo in zip(CHUNKS, halos):
        made, moments = outer_basis(members, halo, moments, firsts, inners, parts)
        outers.update(zip(members, made))
    helm = jnp.pad(helmholtz[None], ((0, 0), (0, LANES - MODES)))
    outers = [outers[n] for n in range(len(SETS))]
    return tuple(solve(of_everyone(moments), helm, firsts, inners, outers))


def solution(mesh):
    in_specs = (P("lev", "tile", None), P(), P("lev"))
    out_specs = (P("lev", "tile", None), P("lev", "tile", None))

    return jax.shard_map(shards, mesh=mesh, in_specs=in_specs, out_specs=out_specs, check_vma=False)
```

```python
import functools

import jax
import jax.numpy as jnp
from jax import lax
from jax.experimental import pallas as pl
from jax.experimental.pallas import tpu as pltpu
from jax.sharding import PartitionSpec as P


STEPS = 8
MOMENTS = 2 * STEPS
ROWS = 16
HALO = 8
MODES = 40
LANES = 128
COLS = 1024
BLOCKS = COLS // LANES
TILES = 64


class ModeSet:
    def __init__(self, *groups):
        self.groups = groups
        self.modes = 8 * len(groups)
        self.base = 8 * groups[0]
        self.segments = LANES // self.modes
        self.length = COLS // self.segments
        self.count = self.length // 8
        self.pitch = self.length + 8

    def rows(self, slabs):
        return slabs * self.pitch + 8


SETS = (ModeSet(0, 1), ModeSet(2, 3), ModeSet(4))
CHUNKS = ((0, 2), (1,))

f32 = jnp.float32
bf16 = jnp.bfloat16


def limits(mib):
    return pltpu.CompilerParams(vmem_limit_bytes=mib * 2**20)


def spread_projection(proj_ref, level0, depth):
    lev = lax.axis_index("lev")
    pick = (
        lax.broadcasted_iota(jnp.int32, (MODES, 2 * MODES), 1)
        == lax.broadcasted_iota(jnp.int32, (MODES, 2 * MODES), 0) + lev * MODES
    ).astype(bf16)
    own = lax.dot_general(
        pick, proj_ref[...], (((1,), (1,)), ((), ())), preferred_element_type=f32
    ).astype(bf16)
    levels = proj_ref.shape[0]
    spread = (
        lax.broadcasted_iota(jnp.int32, (levels, depth), 0)
        == (lax.broadcasted_iota(jnp.int32, (levels, depth), 1) >> 4) + level0
    ).astype(bf16)
    return jnp.dot(own, spread, preferred_element_type=f32)


def build_left(wide, left_refs):
    row_of = lax.broadcasted_iota(jnp.int32, (8, wide.shape[1]), 1) & (ROWS - 1)
    for members, ref in zip(CHUNKS, left_refs):
        at = 0
        for group in groups_of(members):
            part = wide[group * 8:(group + 1) * 8]
            for row in range(0, ROWS, 2):
                two = jnp.concatenate(
                    [jnp.where(row_of == row, part, 0.0), jnp.where(row_of == row + 1, part, 0.0)],
                    axis=0,
                )
                ref[at:at + 16, :] = two.astype(bf16)
                at += 16


def groups_of(members):
    return [group for member in members for group in SETS[member].groups]


def own_levels_kernel(proj_ref, inc_ref, *refs):
    lev = lax.axis_index("lev")
    count = proj_ref.shape[0] // 2
    parts = len(CHUNKS)
    acc_refs, other_refs, left_refs = refs[:parts], refs[parts:2 * parts], refs[2 * parts:]
    depth = left_refs[0].shape[1]

    @pl.when(pl.program_id(0) == 0)
    def _():
        build_left(spread_projection(proj_ref, lev * count, depth), left_refs)

    @pl.when(pl.program_id(0) == pl.num_programs(0) - 1)
    def _():
        build_left(spread_projection(proj_ref, (1 - lev) * count, depth), other_refs)
        for acc_ref, left_ref in zip(acc_refs, left_refs):
            acc_ref[...] = jnp.dot(left_ref[...], inc_ref[...], preferred_element_type=f32)

    @pl.when(pl.program_id(0) < pl.num_programs(0) - 1)
    def _():
        for acc_ref, left_ref in zip(acc_refs, left_refs):
            acc_ref[...] = jnp.dot(left_ref[...], inc_ref[...], preferred_element_type=f32)


def coded(x):
    t = x * 2.0 ** 13
    square = t * t
    eight = t * 8.0
    y = jnp.where(square < 1.0, eight * jnp.abs(eight), (square * 8.0) * ((square * 8.0) * t))
    return y.astype(bf16)


def decoded(y):
    y = y.astype(f32)
    exponent = jnp.log2(jnp.abs(y)) - 6.0
    root = jnp.exp2(exponent * jnp.where(exponent < 0.0, 0.5, 0.2) - 13.0)
    return jnp.where(y < 0.0, -root, root)


def other_levels_kernel(left_ref, inc_ref, acc_ref, modal_ref):
    modal_ref[...] = acc_ref[...] + jnp.dot(
        left_ref[...], inc_ref[...], preferred_element_type=f32
    )


def modal_product(increments, projection):
    levels = increments.shape[0]
    depth = levels * ROWS
    flat = increments.reshape(depth, COLS)
    arrived = lax.ppermute(flat, "lev", [(0, 1), (1, 0)])
    width = 256
    grid = (COLS // width,)
    sizes = [8 * ROWS * len(groups_of(members)) for members in CHUNKS]
    column = lambda rows: pl.BlockSpec((rows, width), lambda c: (0, c))
    whole = lambda rows, cols: pl.BlockSpec((rows, cols), lambda c: (0, 0))
    in_hbm = lambda x: pltpu.with_memory_space_constraint(x, pltpu.HBM)
    made = pl.pallas_call(
        own_levels_kernel,
        grid=grid,
        in_specs=[whole(2 * levels, 2 * MODES), column(depth)],
        out_specs=[column(n) for n in sizes] + [whole(n, depth) for n in sizes],
        out_shape=[jax.ShapeDtypeStruct((n, COLS), f32) for n in sizes]
        + [jax.ShapeDtypeStruct((n, depth), bf16) for n in sizes],
        scratch_shapes=[pltpu.VMEM((n, depth), bf16) for n in sizes],
        compiler_params=limits(20),
        name="own_levels",
    )(in_hbm(projection.T), in_hbm(flat))
    return [
        pl.pallas_call(
            other_levels_kernel,
            grid=grid,
            in_specs=[whole(n, depth), column(depth), column(n)],
            out_specs=column(n),
            out_shape=jax.ShapeDtypeStruct((n, COLS), f32),
            compiler_params=limits(20),
            name="other_levels",
        )(made[len(sizes) + part], arrived, made[part])
        for part, n in enumerate(sizes)
    ]


def lanes():
    return lax.broadcasted_iota(jnp.int32, (8, LANES), 1)


def slab_ends(ref, lead, at, kind, first, last):
    after = pltpu.roll(first, LANES - kind.modes, 1)
    after = jnp.where(lanes() >= LANES - kind.modes, 0.0, after)
    before = jnp.where(lanes() < kind.modes, 0.0, pltpu.roll(last, kind.modes, 1))
    end = at + 8 + kind.length
    ref[lead, end:end + 1, :] = after[0:1, :]
    ref[lead, at + 7:at + 8, :] = before[7:8, :]


def slab_store(ref, lead, at, v, value):
    start = at + 8 + 8 * v
    ref[lead, start:start + value.shape[0], :] = value


def slab_load(ref, lead, at, v, offset=0, count=1):
    start = at + 8 + 8 * v + offset
    if offset == 0 or count == 1:
        return ref[lead, start:start + 8 * count, :]
    parts = [ref[lead, start + 8 * n:start + 8 * n + 8, :] for n in range(count)]
    return jnp.concatenate(parts, axis=0)


def full(shape):
    return pl.BlockSpec(shape, lambda i: (0,) * len(shape))


def single(kernel, outs, mib=16, scratch=()):
    def call(*args):
        return pl.pallas_call(
            kernel,
            grid=(1,),
            in_specs=[full(x.shape) for x in args],
            out_specs=[full(x.shape) for x in outs],
            out_shape=list(outs),
            scratch_shapes=list(scratch),
            compiler_params=limits(mib),
        )(*args)

    return call


def turn_kernel(members, modal_ref, *refs):
    even = (lax.axis_index("tile") & 1) == 0
    first_refs, (a_ref, b_ref) = refs[:len(members)], refs[len(members):]
    places = {group: n for n, group in enumerate(groups_of(members))}
    offset = 0
    for n, member in enumerate(members):
        kind = SETS[member]
        ref = first_refs[n]

        def columns(row):
            parts = []
            for b in range(BLOCKS):
                for group in kind.groups:
                    at = (places[group] * ROWS + row) * 8
                    value = modal_ref[at:at + 8, b * LANES:(b + 1) * LANES]
                    parts.append(value)
                    if len(kind.groups) == 1:
                        parts.append(pltpu.roll(value, LANES // 2, 1))
            return jnp.concatenate(parts, axis=0)

        ready = [columns(row) for row in range(4)]
        for row in range(ROWS):
            whole = ready.pop(0).T
            if row + 4 < ROWS:
                ready.append(columns(row + 4))
            slab_store(ref, 0, row * kind.pitch, 0, whole[:kind.length])
        for row in range(HALO):
            at = offset + row * kind.length
            low, high = [
                coded(slab_load(ref, 0, start * kind.pitch, 0, 0, kind.count))
                for start in (row, row + HALO)
            ]
            a_ref[at:at + kind.length, :] = jnp.where(even, high, low)
            b_ref[at:at + kind.length, :] = jnp.where(even, low, high)
        for row in range(ROWS):
            at = row * kind.pitch
            slab_ends(
                ref, 0, at, kind, slab_load(ref, 0, at, 0), slab_load(ref, 0, at, kind.count - 1)
            )
        offset += HALO * kind.length


def turn(members, modal):
    outs = [jax.ShapeDtypeStruct((1, SETS[m].rows(ROWS), LANES), f32) for m in members]
    edge = sum(HALO * SETS[m].length for m in members)
    outs += [jax.ShapeDtypeStruct((edge, LANES), bf16)] * 2
    out = single(functools.partial(turn_kernel, members), outs)(modal)
    return out[:-2], out[-2:]


def is_inner(order, row):
    return order <= row < ROWS - order


INNER_SLOTS, OUTER_SLOTS = {}, {}
for order_ in range(1, STEPS + 1):
    for row_ in range(ROWS):
        slots_ = INNER_SLOTS if is_inner(order_, row_) else OUTER_SLOTS
        slots_[order_, row_] = len(slots_)
STRIP = 4


def sweep(kind, order, begin, end, place, sums, factor_of):
    for strip in range(0, kind.count, STRIP):
        near = lambda row: slab_load(*place(order - 1, row), strip, 0, STRIP)
        above, here = near(begin - 1), near(begin)
        for row in range(begin, end):
            below = near(row + 1)
            left = slab_load(*place(order - 1, row), strip, -1, STRIP)
            right = slab_load(*place(order - 1, row), strip, 1, STRIP)
            value = ((above + below) + (left + right)) * factor_of(row)
            if order > 1:
                value = value - slab_load(*place(order - 2, row), strip, 0, STRIP)
            ref, lead, at = place(order, row)
            slab_store(ref, lead, at, strip, value)
            if strip + STRIP == kind.count:
                slab_ends(ref, lead, at, kind, slab_load(ref, lead, at, 0), value[-8:])
            if 0 <= row < ROWS:
                if 2 * order < MOMENTS:
                    accumulate(sums, 2 * order, total(value * value))
                accumulate(sums, 2 * order - 1, total(value * here))
            above, here = here, below


def total(values):
    parts = [values[at:at + 8] for at in range(0, values.shape[0], 8)]
    while len(parts) > 1:
        parts = [parts[i] + parts[i + 1] for i in range(0, len(parts), 2)]
    return parts[0]


def accumulate(sums, index, value):
    sums[index] = sums[index] + value if index in sums else value


def inner_kernel(*refs):
    count = len(SETS)
    for kind, first_ref, inner_ref, moment_ref in zip(
        SETS, refs[:count], refs[count:2 * count], refs[2 * count:]
    ):
        def place(order, row):
            if order == 0:
                return first_ref, 0, row * kind.pitch
            return inner_ref, 0, INNER_SLOTS[order, row] * kind.pitch

        sums = {}
        for row in range(ROWS):
            values = slab_load(*place(0, row), 0, 0, kind.count)
            accumulate(sums, 0, total(values * values))
        for order in range(1, STEPS):
            factor = 0.25 if order == 1 else 0.5
            sweep(kind, order, order, ROWS - order, place, sums, lambda row: factor)
        for index in range(MOMENTS):
            if index in sums:
                moment_ref[index:index + 1, :] = jnp.sum(sums[index], axis=0, keepdims=True)
            else:
                moment_ref[index:index + 1, :] = jnp.zeros((1, LANES), f32)


def inner_basis(firsts):
    outs = [jax.ShapeDtypeStruct((1, kind.rows(len(INNER_SLOTS)), LANES), f32) for kind in SETS]
    outs += [jax.ShapeDtypeStruct((MOMENTS, LANES), f32)] * len(SETS)
    out = single(inner_kernel, outs)(*firsts)
    return out[:len(SETS)], out[len(SETS):]


def outer_kernel(members, a_ref, b_ref, known_ref, *refs):
    count = len(members)
    ins, (outs, (moment_ref, *halo_refs)) = refs[:3 * count], (
        refs[3 * count:4 * count], refs[4 * count:]
    )
    tile = lax.axis_index("tile")
    even = (tile & 1) == 0
    half_low = jnp.where(tile == 0, 0.0, 0.5)
    half_high = jnp.where(tile == TILES - 1, 0.0, 0.5)
    lane = lax.broadcasted_iota(jnp.int32, (MOMENTS, LANES), 1)
    moments = known_ref[...]
    offset = 0
    for n, member in enumerate(members):
        kind = SETS[member]
        first_ref, inner_ref, part_ref = ins[3 * n:3 * n + 3]
        outer_ref, halo_ref = outs[n], halo_refs[n]
        for row in range(HALO):
            at = offset + row * kind.length
            a = decoded(a_ref[at:at + kind.length, :])
            b = decoded(b_ref[at:at + kind.length, :])
            for side, value in ((0, jnp.where(even, b, a)), (3, jnp.where(even, a, b))):
                slab_store(halo_ref, side, row * kind.pitch, 0, value)
                slab_ends(halo_ref, side, row * kind.pitch, kind, value[:8], value[-8:])
        offset += HALO * kind.length

        def place(order, row):
            if row < 0:
                return halo_ref, order % 3, (row + HALO) * kind.pitch
            if row >= ROWS:
                return halo_ref, 3 + order % 3, (row - ROWS) * kind.pitch
            if order == 0:
                return first_ref, 0, row * kind.pitch
            if is_inner(order, row):
                return inner_ref, 0, INNER_SLOTS[order, row] * kind.pitch
            return outer_ref, 0, OUTER_SLOTS[order, row] * kind.pitch

        sums = {}
        for order in range(1, STEPS + 1):
            def factor_of(row):
                half = 0.5 if 0 <= row < ROWS else half_low if row < 0 else half_high
                return half * 0.5 if order == 1 else half

            for begin, end in ((order - HALO, order), (ROWS - order, ROWS + HALO - order)):
                sweep(kind, order, begin, end, place, sums, factor_of)
        rows = [
            jnp.sum(sums[i], axis=0, keepdims=True) if i in sums else jnp.zeros((1, LANES), f32)
            for i in range(MOMENTS)
        ]
        part = part_ref[...] + jnp.concatenate(rows, axis=0)
        step = LANES // 2
        while step >= kind.modes:
            part = part + pltpu.roll(part, step, 1)
            step //= 2
        mine = (lane >= kind.base) & (lane < kind.base + kind.modes)
        moments = moments + jnp.where(mine, part, 0.0)
    moment_ref[...] = moments


def outer_basis(members, halo, known, firsts, inners, parts):
    outs = [
        jax.ShapeDtypeStruct((1, SETS[m].rows(len(OUTER_SLOTS)), LANES), f32) for m in members
    ]
    outs += [jax.ShapeDtypeStruct((MOMENTS, LANES), f32)]
    args = [x for m in members for x in (firsts[m], inners[m], parts[m])]
    scratch = [pltpu.VMEM((6, SETS[m].rows(HALO), LANES), f32) for m in members]
    out = single(functools.partial(outer_kernel, members), outs, 24, scratch)(*halo, known, *args)
    return out[:-1], out[-1]


def coefficients(nu, tau):
    half = 0.5 * tau
    rho = list(nu)
    pi = list(nu)
    one = jnp.ones_like(tau)
    r = [one]
    p = [one]
    x = [None] * STEPS
    rr = nu[0]

    def plus(a, b):
        if a is None:
            return b
        if b is None:
            return a
        return a + b

    def inner(c, v):
        terms = [ci * vi for ci, vi in zip(c, v)]
        while len(terms) > 1:
            terms = [sum(terms[i:i + 2]) for i in range(0, len(terms), 2)]
        return terms[0]

    for step in range(STEPS):
        top = MOMENTS - 1 - step
        image = []
        for l in range(top):
            near = pi[l + 1] + pi[abs(l - 1)]
            image.append(pi[l] - half * near)
        alpha = rr / inner(p, image)
        x = [plus(x[i], alpha * p[i]) if i < len(p) else x[i] for i in range(STEPS)]
        shifted = [None] * (len(p) + 1)
        for k, value in enumerate(p):
            if k == 0:
                shifted[1] = plus(shifted[1], tau * value)
            else:
                scaled = half * value
                shifted[k + 1] = plus(shifted[k + 1], scaled)
                shifted[k - 1] = plus(shifted[k - 1], scaled)
        moved = []
        for k in range(len(p) + 1):
            own = p[k] if k < len(p) else None
            if shifted[k] is None:
                moved.append(own)
            elif own is None:
                moved.append(-shifted[k])
            else:
                moved.append(own - shifted[k])
        r = [
            (r[k] - alpha * moved[k]) if k < len(r) else -(alpha * moved[k])
            for k in range(len(moved))
        ]
        if step == STEPS - 1:
            break
        rho = [rho[l] - alpha * image[l] for l in range(top)]
        fresh = inner(r, rho)
        beta = fresh / rr
        pi = [rho[l] + beta * pi[l] for l in range(top)]
        p = [plus(r[k], beta * p[k] if k < len(p) else None) for k in range(len(r))]
        rr = fresh
    return x, r


def solve_kernel(*refs):
    count = len(SETS)
    (own_ref, *term_refs), helm_ref, refs = refs[:4], refs[4], refs[5:]
    fields = [refs[3 * n:3 * n + 3] for n in range(count)]
    x_out, r_out, x_ref, r_ref, mix_ref, stage_ref, coef_ref, sems = refs[3 * count:]
    one, three, two = [ref[...] for ref in term_refs]
    moments = own_ref[...] + (one + three + two)
    raw = [moments[k:k + 1, :] for k in range(MOMENTS)]
    nu = raw[:2]
    for k in range(2, MOMENTS):
        nu.append(2.0 * raw[k] - nu[k & 1])
    x, r = coefficients(nu, 4.0 / (4.0 + helm_ref[...]))
    for k, value in enumerate(x + r):
        coef_ref[k:k + 1, :] = value
    coefs = coef_ref[...]
    lane_all = lax.broadcasted_iota(jnp.int32, coefs.shape, 1)
    low_half = lanes() < LANES // 2
    copies = []
    for kind, (first_ref, inner_ref, outer_ref) in zip(SETS, fields):
        mine = (lane_all >= kind.base) & (lane_all < kind.base + kind.modes)
        own = jnp.where(mine, coefs, 0.0)
        step = kind.modes
        while step < LANES:
            own = own + pltpu.roll(own, step, 1)
            step *= 2
        spread = [jnp.broadcast_to(own[k:k + 1, :], (8, LANES))[None] for k in range(2 * STEPS + 1)]
        cx, cr = spread[:STEPS], spread[STEPS:]

        def combine(row, at):
            for strip in range(0, kind.count, STRIP):
                x = r = None
                for k in range(STEPS + 1):
                    if k == 0:
                        ref, slot = first_ref, row
                    elif is_inner(k, row):
                        ref, slot = inner_ref, INNER_SLOTS[k, row]
                    else:
                        ref, slot = outer_ref, OUTER_SLOTS[k, row]
                    field = slab_load(ref, 0, slot * kind.pitch, strip, 0, STRIP)
                    field = field.reshape(STRIP, 8, LANES)
                    if k < STEPS:
                        x = cx[k] * field if x is None else x + cx[k] * field
                    r = cr[k] * field if r is None else r + cr[k] * field
                for which, value in ((0, x), (1, r)):
                    start = at + 8 * strip
                    mix_ref[which, start:start + 8 * STRIP, :] = value.reshape(8 * STRIP, LANES)

        for top in range(0, ROWS, 8):
            for row in range(8):
                combine(top + row, row * kind.length)
            step = LANES // kind.length
            for row in range(0, 8, step):
                start = row * kind.length
                for which in range(2):
                    both = mix_ref[which, start:start + LANES, :].T
                    if step == 1:
                        stage_ref[which, row] = both
                        continue
                    for b in range(BLOCKS):
                        even = both[16 * b:16 * b + 8]
                        odd = both[16 * b + 8:16 * b + 16]
                        half = LANES // 2
                        stage_ref[which, row, 8 * b:8 * b + 8, :] = jnp.where(
                            low_half, even, pltpu.roll(odd, half, 1)
                        )
                        stage_ref[which, row + 1, 8 * b:8 * b + 8, :] = jnp.where(
                            low_half, pltpu.roll(even, half, 1), odd
                        )
            for which, ref in enumerate((x_ref, r_ref)):
                for b in range(BLOCKS):
                    for n, group in enumerate(kind.groups):
                        at = (b * len(kind.groups) + n) * 8
                        block = jnp.swapaxes(stage_ref[which, :, at:at + 8, :], 0, 1)
                        ref[8 * group:8 * group + 8, top:top + 8, b * LANES:(b + 1) * LANES] = block
        for ref, out in ((x_ref, x_out), (r_ref, r_out)):
            part = pl.ds(kind.base, kind.modes)
            copy = pltpu.make_async_copy(ref.at[part], out.at[part], sems.at[len(copies)])
            copy.start()
            copies.append(copy)
    for copy in copies:
        copy.wait()


def solve(terms, helm, firsts, inners, outers):
    out = jax.ShapeDtypeStruct((MODES, ROWS, COLS), f32)
    args = [*terms, helm] + [x for trio in zip(firsts, inners, outers) for x in trio]
    return pl.pallas_call(
        solve_kernel,
        grid=(1,),
        in_specs=[full(x.shape) for x in args],
        out_specs=[pl.BlockSpec(memory_space=pl.ANY)] * 2,
        out_shape=[out, out],
        scratch_shapes=[
            pltpu.VMEM((MODES, ROWS, COLS), f32),
            pltpu.VMEM((MODES, ROWS, COLS), f32),
            pltpu.VMEM((2, 8 * LANES, LANES), f32),
            pltpu.VMEM((2, 8, LANES, LANES), f32),
            pltpu.VMEM((24, LANES), f32),
            pltpu.SemaphoreType.DMA((2 * len(SETS),)),
        ],
        compiler_params=limits(16),
        name="solve",
    )(*args)


def of_everyone(value):
    for stride in (1, 4, 16):
        one, three, two = [
            lax.ppermute(value, "tile", [(i, i ^ (mask * stride)) for i in range(TILES)])
            for mask in (1, 3, 2)
        ]
        terms = (value, one, three, two)
        value = value + (one + three + two)
    return terms


def shards(increments, projection, helmholtz):
    swap_a = [(i, i ^ 1) for i in range(TILES)]
    swap_b = [(i, i + 1) for i in range(1, TILES - 1, 2)]
    swap_b += [(target, source) for source, target in swap_b]
    firsts, halos = {}, []
    for members, modal in zip(CHUNKS, modal_product(increments, projection)):
        made, (a, b) = turn(members, modal)
        firsts.update(zip(members, made))
        a = lax.ppermute(a, "tile", swap_a)
        b = lax.ppermute(b, "tile", swap_b)
        halos.append((a, b))
    firsts = [firsts[n] for n in range(len(SETS))]
    inners, parts = inner_basis(firsts)
    moments = jnp.zeros((MOMENTS, LANES), f32)
    outers = {}
    for members, halo in zip(CHUNKS, halos):
        made, moments = outer_basis(members, halo, moments, firsts, inners, parts)
        outers.update(zip(members, made))
    helm = jnp.pad(helmholtz[None], ((0, 0), (0, LANES - MODES)))
    outers = [outers[n] for n in range(len(SETS))]
    return tuple(solve(of_everyone(moments), helm, firsts, inners, outers))


def solution(mesh):
    in_specs = (P("lev", "tile", None), P(), P("lev"))
    out_specs = (P("lev", "tile", None), P("lev", "tile", None))

    return jax.shard_map(shards, mesh=mesh, in_specs=in_specs, out_specs=out_specs, check_vma=False)
```
